32 devices in a mesh: dp: 1 (over z), cp: 32 (over y, x, core).
Axes of the slice: x: 4, y: 4, z: 1, core: 2. Of those that a mesh axis runs over, the one named last changes fastest.
The devices are a block of a 4x4x8 slice.
Arguments:
- q_raw: bfloat16 [4096, 64, 128], P(('dp', 'cp'))
- k_raw: bfloat16 [4096, 8, 128], P(('dp', 'cp'))
- v_proj: bfloat16 [4096, 8, 128], P(('dp', 'cp'))
- out_fwd: bfloat16 [4096, 64, 128], P(('dp', 'cp'))
- lse_fwd: float32 [4096, 64], P(('dp', 'cp'))
- d_out: bfloat16 [4096, 64, 128], P(('dp', 'cp'))
- q_norm: float32 [128], replicated
- k_norm: float32 [128], replicated
Outputs:
- output 1: bfloat16 [4096, 64, 128], P(('dp', 'cp'))
- output 2: bfloat16 [4096, 8, 128], P(('dp', 'cp'))
- output 3: bfloat16 [4096, 8, 128], P(('dp', 'cp'))
- output 4: float32 [128], P('dp')
- output 5: float32 [128], P('dp')
All inputs are finite; a program needn't handle non-finite values.
Results may differ from the reference program's by a relative error of at most 0.00271805.
Values are sent between devices in bfloat16 or wider.
A program may use at most 768 MiB of HBM per device.

```python
import jax
import jax.numpy as jnp
from jax import lax

HEADS = 64
KV_HEADS = 8
HEAD_DIM = 128
CHUNK = 64
CP_RANKS = 32
QUERY_BLOCK = 64
SEQ_LEN = 2 * CP_RANKS * CHUNK
Q_PER_KV = HEADS // KV_HEADS
BLOCK_COUNT = SEQ_LEN // QUERY_BLOCK
ROPE_THETA = 1000000.0
NORM_EPS = 1e-6


def layout_positions():
    row_ids = jnp.arange(SEQ_LEN)
    owner_dev = row_ids // (2 * CHUNK)
    within = row_ids % (2 * CHUNK)
    chunk_id = jnp.where(within < CHUNK, owner_dev, 2 * CP_RANKS - 1 - owner_dev)
    return chunk_id * CHUNK + within % CHUNK


def rope_tables(positions):
    inv_freq = ROPE_THETA ** (-jnp.arange(0, HEAD_DIM, 2).astype(jnp.float32) / HEAD_DIM)
    angles = positions.astype(jnp.float32)[:, None] * inv_freq[None, :]
    angles = jnp.concatenate([angles, angles], axis=-1)
    return jnp.cos(angles)[:, None, :], jnp.sin(angles)[:, None, :]


def norm_rope(raw_in, weight, cos_t, sin_t):
    mean_sq = jnp.mean(raw_in * raw_in, axis=-1, keepdims=True)
    normed = raw_in * lax.rsqrt(mean_sq + NORM_EPS) * weight
    half_dim = raw_in.shape[-1] // 2
    rotated = jnp.concatenate([-normed[..., half_dim:], normed[..., :half_dim]], axis=-1)
    return normed * cos_t + rotated * sin_t


def forward_stats(q_raw, k_raw, v_proj, q_norm, k_norm):
    positions = layout_positions()
    cos_t, sin_t = rope_tables(positions)
    q_b = norm_rope(q_raw.astype(jnp.float32), q_norm, cos_t, sin_t).astype(jnp.bfloat16)
    k_b = norm_rope(k_raw.astype(jnp.float32), k_norm, cos_t, sin_t).astype(jnp.bfloat16)
    q_f = q_b.astype(jnp.float32).reshape(BLOCK_COUNT, QUERY_BLOCK, KV_HEADS, Q_PER_KV, HEAD_DIM)
    k_f = k_b.astype(jnp.float32)
    v_f = v_proj.astype(jnp.float32)
    sm_scale = HEAD_DIM ** -0.5

    def one_block(scan_in):
        q_blk, q_pos = scan_in
        logits = jnp.einsum('qngd,knd->qngk', q_blk, k_f) * sm_scale
        visible = (q_pos[:, None] >= positions[None, :])[:, None, None, :]
        logits = jnp.where(visible, logits, -jnp.inf)
        row_max = jnp.max(logits, axis=-1, keepdims=True)
        weights = jnp.exp(logits - row_max)
        row_sum = jnp.sum(weights, axis=-1, keepdims=True)
        out_blk = jnp.einsum('qngk,knd->qngd', weights / row_sum, v_f)
        lse_blk = (row_max + jnp.log(row_sum))[..., 0]
        return out_blk, lse_blk

    out_blocks, lse_blocks = lax.map(one_block, (q_f, positions.reshape(BLOCK_COUNT, QUERY_BLOCK)))
    out_fwd = out_blocks.reshape(SEQ_LEN, HEADS, HEAD_DIM).astype(jnp.bfloat16)
    return out_fwd, lse_blocks.reshape(SEQ_LEN, HEADS)


def setup_inputs(seed: int = 0, part: int = 0) -> dict:
    base_key = jax.random.key(seed)
    shared_key, part_key = jax.random.split(base_key)
    part_key = jax.random.fold_in(part_key, part)
    part_keys = jax.random.split(part_key, 4)
    shared_keys = jax.random.split(shared_key, 2)
    q_raw = jax.random.normal(part_keys[0], (SEQ_LEN, HEADS, HEAD_DIM), jnp.float32).astype(jnp.bfloat16)
    k_raw = jax.random.normal(part_keys[1], (SEQ_LEN, KV_HEADS, HEAD_DIM), jnp.float32).astype(jnp.bfloat16)
    v_proj = jax.random.normal(part_keys[2], (SEQ_LEN, KV_HEADS, HEAD_DIM), jnp.float32).astype(jnp.bfloat16)
    d_out = jax.random.normal(part_keys[3], (SEQ_LEN, HEADS, HEAD_DIM), jnp.float32).astype(jnp.bfloat16)
    q_norm = jax.random.uniform(shared_keys[0], (HEAD_DIM,), jnp.float32, minval=0.5, maxval=1.6)
    k_norm = jax.random.uniform(shared_keys[1], (HEAD_DIM,), jnp.float32, minval=0.5, maxval=1.6)
    out_fwd, lse_fwd = forward_stats(q_raw, k_raw, v_proj, q_norm, k_norm)
    return {'q_raw': q_raw, 'k_raw': k_raw, 'v_proj': v_proj, 'out_fwd': out_fwd, 'lse_fwd': lse_fwd, 'd_out': d_out, 'q_norm': q_norm, 'k_norm': k_norm}


def reference(q_raw, k_raw, v_proj, out_fwd, lse_fwd, d_out, q_norm, k_norm):
    positions = layout_positions()
    cos_t, sin_t = rope_tables(positions)
    q_full, pull_q = jax.vjp(lambda raw_in, weight: norm_rope(raw_in, weight, cos_t, sin_t), q_raw.astype(jnp.float32), q_norm)
    k_full, pull_k = jax.vjp(lambda raw_in, weight: norm_rope(raw_in, weight, cos_t, sin_t), k_raw.astype(jnp.float32), k_norm)
    q_f = q_full.astype(jnp.bfloat16).astype(jnp.float32)
    k_f = k_full.astype(jnp.bfloat16).astype(jnp.float32)
    v_f = v_proj.astype(jnp.float32)
    do_f = d_out.astype(jnp.float32)
    delta_sum = jnp.sum(do_f * out_fwd.astype(jnp.float32), axis=-1)
    sm_scale = HEAD_DIM ** -0.5
    scan_in = (q_f.reshape(BLOCK_COUNT, QUERY_BLOCK, KV_HEADS, Q_PER_KV, HEAD_DIM),
               do_f.reshape(BLOCK_COUNT, QUERY_BLOCK, KV_HEADS, Q_PER_KV, HEAD_DIM),
               lse_fwd.reshape(BLOCK_COUNT, QUERY_BLOCK, KV_HEADS, Q_PER_KV),
               delta_sum.reshape(BLOCK_COUNT, QUERY_BLOCK, KV_HEADS, Q_PER_KV),
               positions.reshape(BLOCK_COUNT, QUERY_BLOCK))

    def scan_step(loop_state, block_in):
        dk_acc, dv_acc = loop_state
        q_blk, do_blk, lse_blk, delta_blk, q_pos = block_in
        logits = jnp.einsum('qngd,knd->qngk', q_blk, k_f) * sm_scale - lse_blk[..., None]
        visible = (q_pos[:, None] >= positions[None, :])[:, None, None, :]
        attn_prob = jnp.exp(jnp.where(visible, logits, -jnp.inf))
        attn_dprob = jnp.einsum('qngd,knd->qngk', do_blk, v_f)
        score_grad = (attn_prob * (attn_dprob - delta_blk[..., None])).astype(jnp.bfloat16).astype(jnp.float32)
        prob_bf = attn_prob.astype(jnp.bfloat16).astype(jnp.float32)
        dq_blk = sm_scale * jnp.einsum('qngk,knd->qngd', score_grad, k_f)
        dk_acc = dk_acc + sm_scale * jnp.einsum('qngk,qngd->knd', score_grad, q_blk)
        dv_acc = dv_acc + jnp.einsum('qngk,qngd->knd', prob_bf, do_blk)
        return (dk_acc, dv_acc), dq_blk

    zero_kv = jnp.zeros((SEQ_LEN, KV_HEADS, HEAD_DIM), jnp.float32)
    (dk_sum, dv_sum), dq_blocks = lax.scan(scan_step, (zero_kv, zero_kv), scan_in)
    dq_raw, dq_norm = pull_q(dq_blocks.reshape(SEQ_LEN, HEADS, HEAD_DIM))
    dk_raw, dk_norm = pull_k(dk_sum)
    return (dq_raw.astype(jnp.bfloat16), dk_raw.astype(jnp.bfloat16), dv_sum.astype(jnp.bfloat16), dq_norm, dk_norm)
```

```python
import functools
import math

import jax
import jax.numpy as jnp
from jax import lax
from jax.experimental import pallas as pl
from jax.experimental.pallas import tpu as pltpu
from jax.sharding import PartitionSpec as P

HEAD_DIM = 128
ROPE_THETA = 1000000.0
NORM_EPS = 1e-6
SM_SCALE = HEAD_DIM ** -0.5
LOG2E = math.log2(math.e)
F32, BF16 = jnp.float32, jnp.bfloat16
NN = (((1,), (0,)), ((), ()))
NT = (((1,), (1,)), ((), ()))
SUB = 16


def rope_tables(positions):
    inv_freq = ROPE_THETA ** (-jnp.arange(0, HEAD_DIM, 2).astype(F32) / HEAD_DIM)
    angles = positions.astype(F32)[:, None] * inv_freq[None, :]
    angles = jnp.concatenate([angles, angles], axis=-1)
    return jnp.cos(angles), jnp.sin(angles)


def norm_rope(raw_in, weight, cos_t, sin_t):
    mean_sq = jnp.mean(raw_in * raw_in, axis=-1, keepdims=True)
    normed = raw_in * lax.rsqrt(mean_sq + NORM_EPS) * weight
    half_dim = raw_in.shape[-1] // 2
    rotated = jnp.concatenate([-normed[..., half_dim:], normed[..., :half_dim]], axis=-1)
    return normed * cos_t + rotated * sin_t


def dot(a, b, dims):
    return lax.dot_general(a, b, dims, preferred_element_type=F32)


def kernel(side, chunk, per_kv, q_hbm, do_hbm, kv_hbm, st_hbm, cos_ref, sin_ref, qn_ref, kn_ref,
           dq_hbm, dkv_hbm, dw_ref,
           qbuf, dobuf, kbuf, stbuf, q_s, do_s, qT, doT, lc, dc, acc, rsbuf, dq_acc, dqo, dko, dwq, dwk, xbuf,
           in_send, kv_send, kv_recv, st_recv, q_recv, do_recv, ag_send, ag_recv, rs_send, rs_recv,
           dq_send, dq_recv, dk_send, dk_recv, x_send, x_recv):
    me = lax.axis_index('cp')
    core = lax.rem(me, 2)
    chip = me // 2
    x = lax.rem(chip, side)
    y = chip // side
    a = (1 - core) * x + core * y
    b = (1 - core) * y + core * x
    head = core * side + a
    top = 2 * side - 1
    rows = 2 * chunk * per_kv
    tile = side * 2 * chunk

    def role_dev(role, ra, rb):
        return ((1 - role) * (rb * side + ra) + role * (ra * side + rb)) * 2 + role

    def dev(d):
        return {'cp': d}

    def remote(src, dst, ssem, rsem, d):
        return pltpu.make_async_remote_copy(src_ref=src, dst_ref=dst, send_sem=ssem, recv_sem=rsem,
                                            device_id=dev(d), device_id_type=pl.DeviceIdType.MESH)

    def landed(ref, sem):
        pltpu.make_async_copy(ref, ref, sem).wait()

    barrier = pltpu.get_barrier_semaphore()
    for dx in range(side):
        for cc in range(2):
            in_row = (y * side + lax.rem(x + dx, side)) * 2 + cc
            in_col = (lax.rem(y + dx, side) * side + x) * 2 + cc
            if dx == 0:
                if cc == 0:
                    pl.semaphore_signal(barrier, inc=1, device_id=dev(chip * 2 + 1 - core), device_id_type=pl.DeviceIdType.MESH)
            else:
                pl.semaphore_signal(barrier, inc=1, device_id=dev(in_row), device_id_type=pl.DeviceIdType.MESH)
                pl.semaphore_signal(barrier, inc=1, device_id=dev(in_col), device_id_type=pl.DeviceIdType.MESH)
    pl.semaphore_wait(barrier, 4 * (side - 1) + 1)

    def in_copies(role, ra, slot):
        hd = role * side + ra
        group = pl.ds(pl.multiple_of(hd * per_kv, per_kv), per_kv)
        kv = []
        for lohi in range(2):
            jj = y if lohi == 0 else top - y
            ii = x if lohi == 0 else side - 1 - x
            half = core if lohi == 0 else 1 - core
            kv.append((kv_hbm.at[hd, lohi], kbuf.at[jj, ii, half], kv_send.at[lohi, role, ra], kv_recv.at[lohi, slot, core]))
        return kv + [(st_hbm.at[hd], stbuf.at[slot, core], in_send.at[0, role, ra], st_recv.at[slot, core]),
                     (q_hbm.at[:, group, :], qbuf.at[slot, core], in_send.at[1, role, ra], q_recv.at[slot, core]),
                     (do_hbm.at[:, group, :], dobuf.at[slot, core], in_send.at[2, role, ra], do_recv.at[slot, core])]

    def coord(role):
        return x if role == 0 else y

    def targets():
        part = 1 - core
        part_a = (1 - part) * x + part * y
        yield part, part_a, part_a, chip * 2 + part
        for dx in (1, side - 1) + tuple(range(2, side - 1)):
            for role in range(2):
                ra = lax.rem(coord(role) + dx, side)
                yield role, ra, coord(role), role_dev(role, ra, y if role == 0 else x)

    own = in_copies(core, a, a)
    sends = []
    for role, ra, slot, d in targets():
        sends.append([remote(s, t, ss, rs, d) for s, t, ss, rs in in_copies(role, ra, slot)])
    for which in ((0, 1), (2, 3, 4)):
        for n in which:
            pltpu.make_async_copy(own[n][0], own[n][1], own[n][3]).start()
        for group in sends:
            for n in which:
                group[n].start()

    acc[...] = jnp.zeros_like(acc)
    dq_acc[...] = jnp.zeros_like(dq_acc)
    dwq[...] = jnp.zeros_like(dwq)
    dwk[...] = jnp.zeros_like(dwk)

    def place(lohi, s, bb):
        ys, xs = (1 - core) * bb + core * s, (1 - core) * s + core * bb
        return (ys, xs) if lohi == 0 else (top - ys, side - 1 - xs)

    ag = []
    for ds in range(side):
        s = lax.rem(a + ds, side)
        for lohi in range(2):
            jj, ii = place(lohi, s, b)
            for cc in range(2):
                landed(kbuf.at[jj, ii, cc], kv_recv.at[lohi, s, cc])
            piece = kbuf.at[jj, ii, :, pl.ds(0, 2)]
            for db in range(1, side):
                cp = remote(piece, piece, ag_send.at[db, lohi, s], ag_recv.at[b, lohi, s],
                            role_dev(core, a, lax.rem(b + db, side)))
                cp.start()
                ag.append(cp)

    def piece_owner(j, i):
        hi = j // side
        jj = j + hi * (top - 2 * j)
        ii = i + hi * (side - 1 - 2 * i)
        return hi, (1 - core) * jj + core * ii, (1 - core) * ii + core * jj

    def block_index(s, lohi):
        cc = (1 - core) * (b * side + s) + core * (s * side + b)
        return cc + lohi * (2 * side * side - 1 - 2 * cc)

    def rope_rows(tref, s, cs, lohi, r0):
        t = tref[s, cs, lohi, pl.ds(r0, SUB), :]
        return jnp.broadcast_to(t[:, None, :], (SUB, per_kv, HEAD_DIM)).reshape(SUB * per_kv, HEAD_DIM)

    def steps(fn):
        n = chunk // SUB

        def body(t, _):
            fn(t, t // n, lax.rem(t, n))
            return 0
        lax.fori_loop(0, 2 * n, body, 0)

    step_rows = SUB * per_kv

    def prepare(s, lohi):
        bi = s * 2 + lohi

        def one(t, cs, sub):
            r0 = pl.multiple_of(sub * SUB, SUB)
            src = pl.ds(pl.multiple_of(lohi * chunk + sub * SUB, SUB), SUB)
            dst = pl.ds(pl.multiple_of(t * step_rows, step_rows), step_rows)
            xq = qbuf[s, cs, src].astype(F32).reshape(step_rows, HEAD_DIM)
            ms = jnp.mean(xq * xq, axis=-1, keepdims=True)
            nq = xq * lax.rsqrt(ms + NORM_EPS) * qn_ref[...]
            qf = nq * rope_rows(cos_ref, s, cs, lohi, r0) + pltpu.roll(nq, HEAD_DIM // 2, 1) * rope_rows(sin_ref, s, cs, lohi, r0)
            q_s[bi, dst, :] = qf.astype(BF16)
            qT[bi, :, dst] = qf.T.astype(BF16)
            dof = dobuf[s, cs, src].astype(F32).reshape(step_rows, HEAD_DIM)
            do_s[bi, dst, :] = dof.astype(BF16)
            doT[bi, :, dst] = dof.T.astype(BF16)
            lanes = pl.ds(pl.multiple_of(sub * step_rows, step_rows), step_rows)
            lc[bi, dst, :] = jnp.broadcast_to(stbuf[s, cs, pl.ds(lohi, 1), lanes], (HEAD_DIM, step_rows)).T
            dc[bi, dst, :] = jnp.broadcast_to(stbuf[s, cs, pl.ds(2 + lohi, 1), lanes], (HEAD_DIM, step_rows)).T
        steps(one)

    def norm_back(g, xr, w, cos_t, sin_t):
        ms = jnp.mean(xr * xr, axis=-1, keepdims=True)
        r = lax.rsqrt(ms + NORM_EPS)
        dn = g * cos_t - pltpu.roll(g, HEAD_DIM // 2, 1) * sin_t
        xh = xr * r
        t = dn * w
        dx = r * (t - xh * jnp.mean(t * xh, axis=-1, keepdims=True))
        return dx, dn * xh

    def finish(s, lohi):
        bi = s * 2 + lohi

        def one(t, cs, sub):
            r0 = pl.multiple_of(sub * SUB, SUB)
            src = pl.ds(pl.multiple_of(lohi * chunk + sub * SUB, SUB), SUB)
            dst = pl.ds(pl.multiple_of(t * step_rows, step_rows), step_rows)
            xq = qbuf[s, cs, src].astype(F32).reshape(step_rows, HEAD_DIM)
            dx, dwt = norm_back(dq_acc[bi, dst, :] * SM_SCALE, xq, qn_ref[...],
                                rope_rows(cos_ref, s, cs, lohi, r0), rope_rows(sin_ref, s, cs, lohi, r0))
            dwq[...] += jnp.sum(dwt.reshape(SUB, 8, HEAD_DIM) if per_kv == 8 else dwt.reshape(step_rows // 8, 8, HEAD_DIM), axis=0)
            dqo[s, cs, src] = dx.reshape(SUB, per_kv, HEAD_DIM).astype(BF16)
        steps(one)
        for cs in range(2):
            part = pl.ds(pl.multiple_of(lohi * chunk, chunk), chunk)
            src = dqo.at[s, cs, part]
            dst = dq_hbm.at[part, pl.ds(pl.multiple_of(head * per_kv, per_kv), per_kv), :]
            target = ((1 - core) * (b * side + s) + core * (s * side + b)) * 2 + cs
            mine = target == me

            @pl.when(mine)
            def _():
                pltpu.make_async_copy(src, dst, dq_recv.at[head, lohi]).start()

            @pl.when(jnp.logical_not(mine))
            def _():
                remote(src, dst, dq_send.at[s, cs, lohi], dq_recv.at[head, lohi], target).start()

    def compute(s, lohi, j, masked):
        bi = s * 2 + lohi
        kt = kbuf[j, :, :, 0].reshape(tile, HEAD_DIM)
        vt = kbuf[j, :, :, 1].reshape(tile, HEAD_DIM)
        z = dot(q_s[bi], kt, NT) * (SM_SCALE * LOG2E) - jnp.tile(lc[bi], (1, tile // HEAD_DIM))
        if masked:
            first = block_index(s, lohi)
            row = lax.broadcasted_iota(jnp.int32, (rows, tile), 0) // per_kv
            half, off = row // chunk, lax.rem(row, chunk)
            half = half + lohi * (1 - 2 * half)
            q_pos = first * (2 * chunk) + half * chunk + off
            k_pos = lax.broadcasted_iota(jnp.int32, (rows, tile), 1) + j * tile
            z = jnp.where(k_pos <= q_pos, z, -jnp.inf)
        p = jnp.exp2(z)
        dp = dot(do_s[bi], vt, NT)
        ds = (p * (dp - jnp.tile(dc[bi], (1, tile // HEAD_DIM)))).astype(BF16)
        pb = p.astype(BF16)
        dv_t = dot(doT[bi], pb, NN)
        dk_t = dot(qT[bi], ds, NN)
        for i in range(side):
            cols = slice(i * 2 * chunk, (i + 1) * 2 * chunk)
            acc[j, i, 0] += dk_t[:, cols]
            acc[j, i, 1] += dv_t[:, cols]
        dq_acc[bi] += dot(ds, kt, NN)

    def rs_copy(j, i, lohi, ob, os):
        return remote(acc.at[j, i], rsbuf.at[b, lohi, os], rs_send.at[j, i], rs_recv.at[b, lohi, os], role_dev(core, a, ob))

    n_group = 2
    per_group = side // n_group

    def group_slot(grp, k):
        n = grp * per_group + k
        return lax.rem(a + n, side)

    def group_body(grp, _):
        def prep_body(k, _):
            s = group_slot(grp, k)
            for cs in range(2):
                landed(stbuf.at[s, cs], st_recv.at[s, cs])
                landed(qbuf.at[s, cs], q_recv.at[s, cs])
                landed(dobuf.at[s, cs], do_recv.at[s, cs])
            prepare(s, 0)
            prepare(s, 1)
            return 0
        lax.fori_loop(0, per_group, prep_body, 0)

        def tile_body(j, _):
            @pl.when(grp == 0)
            def _():
                for i in range(side):
                    lohi, ob, os = piece_owner(j, i)

                    @pl.when(ob != b)
                    def _():
                        landed(kbuf.at[j, i, :, pl.ds(0, 2)], ag_recv.at[ob, lohi, os])

            def block_body(k, _):
                s, lohi = group_slot(grp, k // 2), lax.rem(k, 2)
                full = block_index(s, lohi) // side

                @pl.when(j < full)
                def _():
                    compute(s, lohi, j, False)

                @pl.when(j == full)
                def _():
                    compute(s, lohi, j, True)
                    finish(s, lohi)
                return 0
            lax.fori_loop(0, 2 * per_group, block_body, 0)

            @pl.when(grp == n_group - 1)
            def _():
                for i in range(side):
                    lohi, ob, os = piece_owner(j, i)

                    @pl.when(ob != b)
                    def _():
                        rs_copy(j, i, lohi, ob, os).start()
            return 0
        lax.fori_loop(0, 2 * side, tile_body, 0)
        return 0
    lax.fori_loop(0, n_group, group_body, 0)

    def own_body(t, _):
        lohi, s = t // side, lax.rem(t, side)
        ys, xs = (1 - core) * b + core * s, (1 - core) * s + core * b
        jj = ys + lohi * (top - 2 * ys)
        ii = xs + lohi * (side - 1 - 2 * xs)
        for db in range(1, side):
            ob = lax.rem(b + db, side)
            landed(rsbuf.at[ob, lohi, s], rs_recv.at[ob, lohi, s])
        total = [acc[jj, ii, n] for n in range(2)]
        for db in range(1, side):
            ob = lax.rem(b + db, side)
            total = [total[n] + rsbuf[ob, lohi, s, n] for n in range(2)]
        dk, dv = total[0].T * SM_SCALE, total[1].T
        for half in range(2):
            cs = half + lohi * (1 - 2 * half)
            part = slice(half * chunk, (half + 1) * chunk)
            kr = kbuf[jj, ii, half, 2].astype(F32)
            dx, dwt = norm_back(dk[part], kr, kn_ref[...], cos_ref[s, cs, lohi], sin_ref[s, cs, lohi])
            dwk[...] += jnp.sum(dwt.reshape(chunk // 8, 8, HEAD_DIM), axis=0)
            dko[lohi, s, half, 0] = dx.astype(BF16)
            dko[lohi, s, half, 1] = dv[part].astype(BF16)
            target = ((1 - core) * (b * side + s) + core * (s * side + b)) * 2 + cs
            src, dst = dko.at[lohi, s, half], dkv_hbm.at[head, lohi]
            mine = target == me

            @pl.when(mine)
            def _():
                pltpu.make_async_copy(src, dst, dk_recv.at[head, lohi]).start()

            @pl.when(jnp.logical_not(mine))
            def _():
                remote(src, dst, dk_send.at[lohi, s, half], dk_recv.at[head, lohi], target).start()
        return 0
    lax.fori_loop(0, 2 * side, own_body, 0)

    xbuf[0, a, 0] = dwq[...]
    xbuf[0, a, 1] = dwk[...]
    for stage in range(2):
        pos = (a, b)[stage]
        cps = []
        for d in range(1, side):
            o = lax.rem(pos + d, side)
            other = role_dev(core, o, b) if stage == 0 else role_dev(core, a, o)
            cp = remote(xbuf.at[stage, pos], xbuf.at[stage, pos], x_send.at[stage, d], x_recv.at[stage, pos], other)
            cp.start()
            cps.append(cp)
        for d in range(1, side):
            o = lax.rem(pos + d, side)
            landed(xbuf.at[stage, o], x_recv.at[stage, o])
        total = xbuf[stage, 0]
        for o in range(1, side):
            total = total + xbuf[stage, o]
        for cp in cps:
            cp.wait_send()
        if stage == 0:
            xbuf[1, b] = total
        else:
            xbuf[2, core] = total
    cp = remote(xbuf.at[2, core], xbuf.at[2, core], x_send.at[2, 0], x_recv.at[2, core], chip * 2 + 1 - core)
    cp.start()
    landed(xbuf.at[2, 1 - core], x_recv.at[2, 1 - core])
    dw_ref[...] = xbuf[2, 0] + xbuf[2, 1]
    cp.wait_send()

    for group in sends:
        for cp in group:
            cp.wait_send()
    for cp in ag:
        cp.wait_send()

    def drain_rs(j, _):
        for i in range(side):
            lohi, ob, os = piece_owner(j, i)

            @pl.when(ob != b)
            def _():
                rs_copy(j, i, lohi, ob, os).wait_send()
        return 0
    lax.fori_loop(0, 2 * side, drain_rs, 0)

    def drain_out(t, _):
        s, lohi = t // 2, lax.rem(t, 2)
        for cs in range(2):
            target = ((1 - core) * (b * side + s) + core * (s * side + b)) * 2 + cs
            half = cs + lohi * (1 - 2 * cs)

            @pl.when(target != me)
            def _():
                part = dqo.at[s, cs, pl.ds(0, chunk)]
                pltpu.make_async_copy(part, part, dq_send.at[s, cs, lohi]).wait()
                part = dko.at[lohi, s, half]
                pltpu.make_async_copy(part, part, dk_send.at[lohi, s, half]).wait()
        return 0
    lax.fori_loop(0, 2 * side, drain_out, 0)

    def drain_in(t, _):
        hd, lohi = t // 2, lax.rem(t, 2)
        part = pl.ds(pl.multiple_of(lohi * chunk, chunk), chunk)
        landed(dq_hbm.at[part, pl.ds(pl.multiple_of(hd * per_kv, per_kv), per_kv), :], dq_recv.at[hd, lohi])
        landed(dkv_hbm.at[hd, lohi], dk_recv.at[hd, lohi])
        return 0
    lax.fori_loop(0, 4 * side, drain_in, 0)


def solution(mesh):
    cp_size = mesh.shape['cp']
    side = math.isqrt(cp_size // 2)

    def local_grads(q_raw, k_raw, v_proj, out_fwd, lse_fwd, d_out, q_norm, k_norm):
        me = lax.axis_index('cp')
        local_rows, num_heads = q_raw.shape[0], q_raw.shape[1]
        chunk = local_rows // 2
        kv_heads = k_raw.shape[1]
        per_kv = num_heads // kv_heads
        core, chip = me % 2, me // 2
        x, y = chip % side, chip // side

        offs = jnp.arange(chunk)

        def chunk_positions(device):
            return jnp.stack([device * chunk + offs, (2 * cp_size - 1 - device) * chunk + offs], axis=-2)

        cos_k, sin_k = rope_tables(chunk_positions(me).reshape(-1))
        k_b = norm_rope(k_raw.astype(F32), k_norm, cos_k[:, None, :], sin_k[:, None, :]).astype(BF16)
        kv = jnp.stack([k_b, v_proj, k_raw]).reshape(3, 2, chunk, kv_heads, HEAD_DIM).transpose(3, 1, 0, 2, 4)
        delta = jnp.sum(d_out.astype(F32) * out_fwd.astype(F32), axis=-1)
        stats = jnp.stack([lse_fwd * LOG2E, delta]).reshape(2, 2, chunk, kv_heads, per_kv)
        stats = stats.transpose(3, 0, 1, 2, 4).reshape(kv_heads, 4, chunk * per_kv)

        slots = jnp.arange(side)
        src_chip = jnp.where(core == 0, y * side + slots, slots * side + x)
        src_dev = src_chip[:, None] * 2 + jnp.arange(2)[None, :]
        pos = chunk_positions(src_dev[:, :, None, None])
        cos_t, sin_t = rope_tables(pos.reshape(-1))
        sign = jnp.where(jnp.arange(HEAD_DIM) < HEAD_DIM // 2, -1.0, 1.0).astype(F32)
        cos_t = cos_t.reshape(side, 2, 2, chunk, HEAD_DIM)
        sin_t = (sin_t * sign).reshape(side, 2, 2, chunk, HEAD_DIM)

        rows = local_rows * per_kv
        dma = pltpu.SemaphoreType.DMA
        any_spec, vmem_spec = pl.BlockSpec(memory_space=pl.ANY), pl.BlockSpec(memory_space=pltpu.VMEM)
        dq_raw, dkv, dw = pl.pallas_call(
            functools.partial(kernel, side, chunk, per_kv),
            out_shape=(jax.ShapeDtypeStruct(q_raw.shape, BF16),
                       jax.ShapeDtypeStruct((kv_heads, 2, 2, chunk, HEAD_DIM), BF16),
                       jax.ShapeDtypeStruct((2, 8, HEAD_DIM), F32)),
            in_specs=[any_spec] * 4 + [vmem_spec] * 4,
            out_specs=(any_spec, any_spec, vmem_spec),
            scratch_shapes=[
                pltpu.VMEM((side, 2, local_rows, per_kv, HEAD_DIM), BF16),
                pltpu.VMEM((side, 2, local_rows, per_kv, HEAD_DIM), BF16),
                pltpu.VMEM((2 * side, side, 2, 3, chunk, HEAD_DIM), BF16),
                pltpu.VMEM((side, 2, 4, chunk * per_kv), F32),
                pltpu.VMEM((2 * side, rows, HEAD_DIM), BF16),
                pltpu.VMEM((2 * side, rows, HEAD_DIM), BF16),
                pltpu.VMEM((2 * side, HEAD_DIM, rows), BF16),
                pltpu.VMEM((2 * side, HEAD_DIM, rows), BF16),
                pltpu.VMEM((2 * side, rows, HEAD_DIM), F32),
                pltpu.VMEM((2 * side, rows, HEAD_DIM), F32),
                pltpu.VMEM((2 * side, side, 2, HEAD_DIM, 2 * chunk), F32),
                pltpu.VMEM((side, 2, side, 2, HEAD_DIM, 2 * chunk), F32),
                pltpu.VMEM((2 * side, rows, HEAD_DIM), F32),
                pltpu.VMEM((side, 2, local_rows, per_kv, HEAD_DIM), BF16),
                pltpu.VMEM((2, side, 2, 2, chunk, HEAD_DIM), BF16),
                pltpu.VMEM((8, HEAD_DIM), F32),
                pltpu.VMEM((8, HEAD_DIM), F32),
                pltpu.VMEM((3, side, 2, 8, HEAD_DIM), F32),
                dma((3, 2, side)), dma((2, 2, side)), dma((2, side, 2)), dma((side, 2)), dma((side, 2)), dma((side, 2)),
                dma((side, 2, side)), dma((side, 2, side)), dma((2 * side, side)), dma((side, 2, side)),
                dma((side, 2, 2)), dma((kv_heads, 2)), dma((2, side, 2)), dma((kv_heads, 2)),
                dma((3, side)), dma((3, side)),
            ],
            compiler_params=pltpu.CompilerParams(collective_id=0, has_side_effects=True, vmem_limit_bytes=60 << 20),
            name='attention_backward',
        )(q_raw, d_out, kv, stats, cos_t, sin_t, q_norm[None, :], k_norm[None, :])
        dkv = dkv.transpose(2, 1, 3, 0, 4).reshape(2, local_rows, kv_heads, HEAD_DIM)
        dw = jnp.sum(dw, axis=1)
        return dq_raw, dkv[0], dkv[1], dw[0], dw[1]

    row_spec = P(('dp', 'cp'))
    in_specs = (row_spec, row_spec, row_spec, row_spec, row_spec, row_spec, P(), P())
    out_specs = (row_spec, row_spec, row_spec, P('dp'), P('dp'))
    return jax.shard_map(local_grads, mesh=mesh, in_specs=in_specs, out_specs=out_specs, check_vma=False)
```

```python
import functools
import math

import jax
import jax.numpy as jnp
from jax import lax
from jax.experimental import pallas as pl
from jax.experimental.pallas import tpu as pltpu
from jax.sharding import PartitionSpec as P

HEAD_DIM = 128
ROPE_THETA = 1000000.0
NORM_EPS = 1e-6
SM_SCALE = HEAD_DIM ** -0.5
LOG2E = math.log2(math.e)
F32, BF16 = jnp.float32, jnp.bfloat16
NN = (((1,), (0,)), ((), ()))
NT = (((1,), (1,)), ((), ()))
SUB = 32


def rope_tables(positions):
    inv_freq = ROPE_THETA ** (-jnp.arange(0, HEAD_DIM, 2).astype(F32) / HEAD_DIM)
    angles = positions.astype(F32)[:, None] * inv_freq[None, :]
    angles = jnp.concatenate([angles, angles], axis=-1)
    return jnp.cos(angles), jnp.sin(angles)


def norm_rope(raw_in, weight, cos_t, sin_t):
    mean_sq = jnp.mean(raw_in * raw_in, axis=-1, keepdims=True)
    normed = raw_in * lax.rsqrt(mean_sq + NORM_EPS) * weight
    half_dim = raw_in.shape[-1] // 2
    rotated = jnp.concatenate([-normed[..., half_dim:], normed[..., :half_dim]], axis=-1)
    return normed * cos_t + rotated * sin_t


def dot(a, b, dims):
    return lax.dot_general(a, b, dims, preferred_element_type=F32)


def kernel(side, chunk, per_kv, q_hbm, do_hbm, kv_hbm, st_hbm, cos_ref, sin_ref, qn_ref, kn_ref,
           dq_hbm, dkv_hbm, dw_ref,
           qbuf, dobuf, kbuf, stbuf, q_s, do_s, qT, doT, lc, dc, rb, acc, rsbuf, dq_acc, dqo, dko, dwq, dwk, xbuf,
           in_send, kv_send, kv_recv, st_recv, q_recv, do_recv, ag_send, ag_recv, rs_send, rs_recv,
           dq_send, dq_recv, dk_send, dk_recv, x_send, x_recv):
    me = lax.axis_index('cp')
    core = lax.rem(me, 2)
    chip = me // 2
    x = lax.rem(chip, side)
    y = chip // side
    a = (1 - core) * x + core * y
    b = (1 - core) * y + core * x
    head = core * side + a
    top = 2 * side - 1
    local_rows = 2 * chunk
    rows = 2 * chunk * per_kv
    tile = side * 2 * chunk

    def role_dev(role, ra, rb):
        return ((1 - role) * (rb * side + ra) + role * (ra * side + rb)) * 2 + role

    def dev(d):
        return {'cp': d}

    def remote(src, dst, ssem, rsem, d):
        return pltpu.make_async_remote_copy(src_ref=src, dst_ref=dst, send_sem=ssem, recv_sem=rsem,
                                            device_id=dev(d), device_id_type=pl.DeviceIdType.MESH)

    def landed(ref, sem):
        pltpu.make_async_copy(ref, ref, sem).wait()

    barrier = pltpu.get_barrier_semaphore()
    for dx in range(side):
        for cc in range(2):
            in_row = (y * side + lax.rem(x + dx, side)) * 2 + cc
            in_col = (lax.rem(y + dx, side) * side + x) * 2 + cc
            if dx == 0:
                if cc == 0:
                    pl.semaphore_signal(barrier, inc=1, device_id=dev(chip * 2 + 1 - core), device_id_type=pl.DeviceIdType.MESH)
            else:
                pl.semaphore_signal(barrier, inc=1, device_id=dev(in_row), device_id_type=pl.DeviceIdType.MESH)
                pl.semaphore_signal(barrier, inc=1, device_id=dev(in_col), device_id_type=pl.DeviceIdType.MESH)
    pl.semaphore_wait(barrier, 4 * (side - 1) + 1)

    def in_copies(role, ra, slot):
        hd = role * side + ra
        group = pl.ds(pl.multiple_of(hd * per_kv, per_kv), per_kv)
        kv = []
        for lohi in range(2):
            jj = y if lohi == 0 else top - y
            ii = x if lohi == 0 else side - 1 - x
            half = core if lohi == 0 else 1 - core
            kv.append((kv_hbm.at[hd, lohi], kbuf.at[jj, ii, half], kv_send.at[lohi, role, ra], kv_recv.at[lohi, slot, core]))
        return kv + [(st_hbm.at[hd], stbuf.at[slot, core], in_send.at[0, role, ra], st_recv.at[slot, core]),
                     (q_hbm.at[:, group, :], qbuf.at[slot, core], in_send.at[1, role, ra], q_recv.at[slot, core]),
                     (do_hbm.at[:, group, :], dobuf.at[slot, core], in_send.at[2, role, ra], do_recv.at[slot, core])]

    def coord(role):
        return x if role == 0 else y

    def targets():
        part = 1 - core
        part_a = (1 - part) * x + part * y
        yield part, part_a, part_a, chip * 2 + part
        for dx in (1, side - 1) + tuple(range(2, side - 1)):
            for role in range(2):
                ra = lax.rem(coord(role) + dx, side)
                yield role, ra, coord(role), role_dev(role, ra, y if role == 0 else x)

    own = in_copies(core, a, a)
    sends = []
    for role, ra, slot, d in targets():
        sends.append([remote(s, t, ss, rs, d) for s, t, ss, rs in in_copies(role, ra, slot)])
    def start_own(which):
        for n in which:
            pltpu.make_async_copy(own[n][0], own[n][1], own[n][3]).start()

    def start_sends(groups, which):
        for group in groups:
            for n in which:
                group[n].start()

    start_own((0, 1))
    start_sends(sends, (0, 1))
    start_own((2, 3, 4))
    start_sends(sends[:1], (2, 3, 4))

    acc[...] = jnp.zeros_like(acc)
    dq_acc[...] = jnp.zeros_like(dq_acc)
    dwq[...] = jnp.zeros_like(dwq)
    dwk[...] = jnp.zeros_like(dwk)

    def place(lohi, s, bb):
        ys, xs = (1 - core) * bb + core * s, (1 - core) * s + core * bb
        return (ys, xs) if lohi == 0 else (top - ys, side - 1 - xs)

    ag = []
    for ds in range(side):
        s = lax.rem(a + ds, side)
        for lohi in range(2):
            jj, ii = place(lohi, s, b)
            for cc in range(2):
                landed(kbuf.at[jj, ii, cc], kv_recv.at[lohi, s, cc])
            piece = kbuf.at[jj, ii, :, pl.ds(0, 2)]
            for db in range(1, side):
                cp = remote(piece, piece, ag_send.at[db, lohi, s], ag_recv.at[b, lohi, s],
                            role_dev(core, a, lax.rem(b + db, side)))
                cp.start()
                ag.append(cp)

    for cp in ag:
        cp.wait_send()
    start_sends(sends[1:], (2, 3, 4))

    def piece_owner(j, i):
        hi = j // side
        jj = j + hi * (top - 2 * j)
        ii = i + hi * (side - 1 - 2 * i)
        return hi, (1 - core) * jj + core * ii, (1 - core) * ii + core * jj

    def block_index(s, lohi):
        cc = (1 - core) * (b * side + s) + core * (s * side + b)
        return cc + lohi * (2 * side * side - 1 - 2 * cc)

    def rope_rows(tref, s, cs, lohi, r0):
        view = tref.at[s, cs, lohi]
        return jnp.concatenate([view[pl.ds(r0 + i, per_kv, stride=0), :] for i in range(SUB)], axis=0)

    def stat_rows(n, s, cs, first):
        t = pltpu.roll(stbuf[s, cs, n], local_rows - first, 1)
        return jnp.concatenate([jnp.broadcast_to(t[:, i:i + 1], (per_kv, HEAD_DIM)) for i in range(SUB)], axis=0)

    def steps(fn):
        n = chunk // SUB

        def body(t, _):
            fn(t, t // n, lax.rem(t, n))
            return 0
        lax.fori_loop(0, 2 * n, body, 0)

    step_rows = SUB * per_kv

    def prepare(s, lohi):
        bi = s * 2 + lohi

        def one(t, cs, sub):
            r0 = pl.multiple_of(sub * SUB, SUB)
            src = pl.ds(pl.multiple_of(lohi * chunk + sub * SUB, SUB), SUB)
            dst = pl.ds(pl.multiple_of(t * step_rows, step_rows), step_rows)
            xq = qbuf[s, cs, src].astype(F32).reshape(step_rows, HEAD_DIM)
            ms = jnp.mean(xq * xq, axis=-1, keepdims=True)
            r = jnp.broadcast_to(lax.rsqrt(ms + NORM_EPS), xq.shape)
            rb[bi, dst, :] = r
            nq = xq * r * qn_ref[...]
            qf = nq * rope_rows(cos_ref, s, cs, lohi, r0) + pltpu.roll(nq, HEAD_DIM // 2, 1) * rope_rows(sin_ref, s, cs, lohi, r0)
            qf = qf.astype(BF16)
            q_s[bi, dst, :] = qf
            qT[bi, :, dst] = qf.T
            dof = dobuf[s, cs, src].astype(F32).reshape(step_rows, HEAD_DIM)
            dof = dof.astype(BF16)
            do_s[bi, dst, :] = dof
            doT[bi, :, dst] = dof.T
            lc[bi, dst, :] = stat_rows(0, s, cs, lohi * chunk + sub * SUB)
            dc[bi, dst, :] = stat_rows(1, s, cs, lohi * chunk + sub * SUB)
        steps(one)

    def inv_rms(xr):
        return lax.rsqrt(jnp.mean(xr * xr, axis=-1, keepdims=True) + NORM_EPS)

    def norm_back(g, xr, r, w, cos_t, sin_t):
        dn = g * cos_t - pltpu.roll(g, HEAD_DIM // 2, 1) * sin_t
        xh = xr * r
        t = dn * w
        dx = r * (t - xh * jnp.mean(t * xh, axis=-1, keepdims=True))
        return dx, dn * xh

    def finish(s, lohi):
        bi = s * 2 + lohi

        def one(t, cs, sub):
            r0 = pl.multiple_of(sub * SUB, SUB)
            src = pl.ds(pl.multiple_of(lohi * chunk + sub * SUB, SUB), SUB)
            dst = pl.ds(pl.multiple_of(t * step_rows, step_rows), step_rows)
            xq = qbuf[s, cs, src].astype(F32).reshape(step_rows, HEAD_DIM)
            dx, dwt = norm_back(dq_acc[bi, dst, :] * SM_SCALE, xq, rb[bi, dst, :], qn_ref[...],
                                rope_rows(cos_ref, s, cs, lohi, r0), rope_rows(sin_ref, s, cs, lohi, r0))
            dwq[...] += jnp.sum(dwt.reshape(step_rows // 8, 8, HEAD_DIM), axis=0)
            dqo[s, cs, src] = dx.reshape(SUB, per_kv, HEAD_DIM).astype(BF16)
        steps(one)
        for cs in range(2):
            part = pl.ds(pl.multiple_of(lohi * chunk, chunk), chunk)
            src = dqo.at[s, cs, part]
            dst = dq_hbm.at[part, pl.ds(pl.multiple_of(head * per_kv, per_kv), per_kv), :]
            target = ((1 - core) * (b * side + s) + core * (s * side + b)) * 2 + cs
            mine = target == me

            @pl.when(mine)
            def _():
                pltpu.make_async_copy(src, dst, dq_recv.at[head, lohi]).start()

            @pl.when(jnp.logical_not(mine))
            def _():
                remote(src, dst, dq_send.at[s, cs, lohi], dq_recv.at[head, lohi], target).start()

    def compute(s, lohi, j, masked):
        bi = s * 2 + lohi
        kt = kbuf[j, :, :, 0].reshape(tile, HEAD_DIM)
        vt = kbuf[j, :, :, 1].reshape(tile, HEAD_DIM)
        z = dot(q_s[bi], kt, NT) * (SM_SCALE * LOG2E) - jnp.tile(lc[bi], (1, tile // HEAD_DIM))
        if masked:
            first = block_index(s, lohi)
            row = lax.broadcasted_iota(jnp.int32, (rows, tile), 0) // per_kv
            half, off = row // chunk, lax.rem(row, chunk)
            half = half + lohi * (1 - 2 * half)
            q_pos = first * (2 * chunk) + half * chunk + off
            k_pos = lax.broadcasted_iota(jnp.int32, (rows, tile), 1) + j * tile
            z = jnp.where(k_pos <= q_pos, z, -jnp.inf)
        p = jnp.exp2(z)
        dp = dot(do_s[bi], vt, NT)
        ds = (p * (dp - jnp.tile(dc[bi], (1, tile // HEAD_DIM)))).astype(BF16)
        pb = p.astype(BF16)
        dv_t = dot(doT[bi], pb, NN)
        dk_t = dot(qT[bi], ds, NN)
        for i in range(side):
            cols = slice(i * 2 * chunk, (i + 1) * 2 * chunk)
            acc[j, i, 0] += dk_t[:, cols]
            acc[j, i, 1] += dv_t[:, cols]
        dq_acc[bi] += dot(ds, kt, NN)

    def rs_copy(j, i, lohi, ob, os):
        return remote(acc.at[j, i], rsbuf.at[b, lohi, os], rs_send.at[j, i], rs_recv.at[b, lohi, os], role_dev(core, a, ob))

    n_group = 3

    def group_slot(grp, k):
        n = grp + k
        return lax.rem(a + n + (n // 2) * (side + 1 - 2 * n), side)

    def group_body(grp, _):
        per_group = 1 + grp // 2

        def prep_body(k, _):
            s = group_slot(grp, k)
            for cs in range(2):
                landed(stbuf.at[s, cs], st_recv.at[s, cs])
                landed(qbuf.at[s, cs], q_recv.at[s, cs])
                landed(dobuf.at[s, cs], do_recv.at[s, cs])
            prepare(s, 0)
            prepare(s, 1)
            return 0
        lax.fori_loop(0, per_group, prep_body, 0)

        def tile_body(j, _):
            @pl.when(grp == 0)
            def _():
                for i in range(side):
                    lohi, ob, os = piece_owner(j, i)

                    @pl.when(ob != b)
                    def _():
                        landed(kbuf.at[j, i, :, pl.ds(0, 2)], ag_recv.at[ob, lohi, os])

            def block_body(k, _):
                s, lohi = group_slot(grp, k // 2), lax.rem(k, 2)
                full = block_index(s, lohi) // side

                @pl.when(j < full)
                def _():
                    compute(s, lohi, j, False)

                @pl.when(j == full)
                def _():
                    compute(s, lohi, j, True)
                    finish(s, lohi)
                return 0
            lax.fori_loop(0, 2 * per_group, block_body, 0)

            @pl.when(grp == n_group - 1)
            def _():
                for i in range(side):
                    lohi, ob, os = piece_owner(j, i)

                    @pl.when(ob != b)
                    def _():
                        rs_copy(j, i, lohi, ob, os).start()
            return 0
        lax.fori_loop(0, 2 * side, tile_body, 0)
        return 0
    lax.fori_loop(0, n_group, group_body, 0)

    def own_body(t, _):
        lohi, s = t // side, lax.rem(t, side)
        ys, xs = (1 - core) * b + core * s, (1 - core) * s + core * b
        jj = ys + lohi * (top - 2 * ys)
        ii = xs + lohi * (side - 1 - 2 * xs)
        for db in range(1, side):
            ob = lax.rem(b + db, side)
            landed(rsbuf.at[ob, lohi, s], rs_recv.at[ob, lohi, s])
        total = [acc[jj, ii, n] for n in range(2)]
        for db in range(1, side):
            ob = lax.rem(b + db, side)
            total = [total[n] + rsbuf[ob, lohi, s, n] for n in range(2)]
        dk, dv = total[0].T * SM_SCALE, total[1].T
        for half in range(2):
            cs = half + lohi * (1 - 2 * half)
            part = slice(half * chunk, (half + 1) * chunk)
            kr = kbuf[jj, ii, half, 2].astype(F32)
            dx, dwt = norm_back(dk[part], kr, inv_rms(kr), kn_ref[...], cos_ref[s, cs, lohi], sin_ref[s, cs, lohi])
            dwk[...] += jnp.sum(dwt.reshape(chunk // 8, 8, HEAD_DIM), axis=0)
            dko[lohi, s, half, 0] = dx.astype(BF16)
            dko[lohi, s, half, 1] = dv[part].astype(BF16)
            target = ((1 - core) * (b * side + s) + core * (s * side + b)) * 2 + cs
            src, dst = dko.at[lohi, s, half], dkv_hbm.at[head, lohi]
            mine = target == me

            @pl.when(mine)
            def _():
                pltpu.make_async_copy(src, dst, dk_recv.at[head, lohi]).start()

            @pl.when(jnp.logical_not(mine))
            def _():
                remote(src, dst, dk_send.at[lohi, s, half], dk_recv.at[head, lohi], target).start()
        return 0
    lax.fori_loop(0, 2 * side, own_body, 0)

    xbuf[0, a, 0] = dwq[...]
    xbuf[0, a, 1] = dwk[...]
    for stage in range(2):
        pos = (a, b)[stage]
        cps = []
        for d in range(1, side):
            o = lax.rem(pos + d, side)
            other = role_dev(core, o, b) if stage == 0 else role_dev(core, a, o)
            cp = remote(xbuf.at[stage, pos], xbuf.at[stage, pos], x_send.at[stage, d], x_recv.at[stage, pos], other)
            cp.start()
            cps.append(cp)
        for d in range(1, side):
            o = lax.rem(pos + d, side)
            landed(xbuf.at[stage, o], x_recv.at[stage, o])
        total = xbuf[stage, 0]
        for o in range(1, side):
            total = total + xbuf[stage, o]
        for cp in cps:
            cp.wait_send()
        if stage == 0:
            xbuf[1, b] = total
        else:
            xbuf[2, core] = total
    cp = remote(xbuf.at[2, core], xbuf.at[2, core], x_send.at[2, 0], x_recv.at[2, core], chip * 2 + 1 - core)
    cp.start()
    landed(xbuf.at[2, 1 - core], x_recv.at[2, 1 - core])
    dw_ref[...] = xbuf[2, 0] + xbuf[2, 1]
    cp.wait_send()

    for group in sends:
        for cp in group:
            cp.wait_send()
    def drain_rs(j, _):
        for i in range(side):
            lohi, ob, os = piece_owner(j, i)

            @pl.when(ob != b)
            def _():
                rs_copy(j, i, lohi, ob, os).wait_send()
        return 0
    lax.fori_loop(0, 2 * side, drain_rs, 0)

    def drain_out(t, _):
        s, lohi = t // 2, lax.rem(t, 2)
        for cs in range(2):
            target = ((1 - core) * (b * side + s) + core * (s * side + b)) * 2 + cs
            half = cs + lohi * (1 - 2 * cs)

            @pl.when(target != me)
            def _():
                part = dqo.at[s, cs, pl.ds(0, chunk)]
                pltpu.make_async_copy(part, part, dq_send.at[s, cs, lohi]).wait()
                part = dko.at[lohi, s, half]
                pltpu.make_async_copy(part, part, dk_send.at[lohi, s, half]).wait()
        return 0
    lax.fori_loop(0, 2 * side, drain_out, 0)

    def drain_in(t, _):
        hd, lohi = t // 2, lax.rem(t, 2)
        part = pl.ds(pl.multiple_of(lohi * chunk, chunk), chunk)
        landed(dq_hbm.at[part, pl.ds(pl.multiple_of(hd * per_kv, per_kv), per_kv), :], dq_recv.at[hd, lohi])
        landed(dkv_hbm.at[hd, lohi], dk_recv.at[hd, lohi])
        return 0
    lax.fori_loop(0, 4 * side, drain_in, 0)


def solution(mesh):
    cp_size = mesh.shape['cp']
    side = math.isqrt(cp_size // 2)

    def local_grads(q_raw, k_raw, v_proj, out_fwd, lse_fwd, d_out, q_norm, k_norm):
        me = lax.axis_index('cp')
        local_rows, num_heads = q_raw.shape[0], q_raw.shape[1]
        chunk = local_rows // 2
        kv_heads = k_raw.shape[1]
        per_kv = num_heads // kv_heads
        core, chip = me % 2, me // 2
        x, y = chip % side, chip // side

        offs = jnp.arange(chunk)

        def chunk_positions(device):
            return jnp.stack([device * chunk + offs, (2 * cp_size - 1 - device) * chunk + offs], axis=-2)

        cos_k, sin_k = rope_tables(chunk_positions(me).reshape(-1))
        k_b = norm_rope(k_raw.astype(F32), k_norm, cos_k[:, None, :], sin_k[:, None, :]).astype(BF16)
        kv = jnp.stack([k_b, v_proj, k_raw]).reshape(3, 2, chunk, kv_heads, HEAD_DIM).transpose(3, 1, 0, 2, 4)
        delta = jnp.sum(d_out.astype(F32) * out_fwd.astype(F32), axis=-1)
        stats = jnp.stack([lse_fwd * LOG2E, delta]).reshape(2, local_rows, kv_heads, per_kv)
        stats = stats.transpose(2, 0, 3, 1)

        slots = jnp.arange(side)
        src_chip = jnp.where(core == 0, y * side + slots, slots * side + x)
        src_dev = src_chip[:, None] * 2 + jnp.arange(2)[None, :]
        pos = chunk_positions(src_dev[:, :, None, None])
        cos_t, sin_t = rope_tables(pos.reshape(-1))
        sign = jnp.where(jnp.arange(HEAD_DIM) < HEAD_DIM // 2, -1.0, 1.0).astype(F32)
        cos_t = cos_t.reshape(side, 2, 2, chunk, HEAD_DIM)
        sin_t = (sin_t * sign).reshape(side, 2, 2, chunk, HEAD_DIM)

        rows = local_rows * per_kv
        dma = pltpu.SemaphoreType.DMA
        any_spec, vmem_spec = pl.BlockSpec(memory_space=pl.ANY), pl.BlockSpec(memory_space=pltpu.VMEM)
        dq_raw, dkv, dw = pl.pallas_call(
            functools.partial(kernel, side, chunk, per_kv),
            out_shape=(jax.ShapeDtypeStruct(q_raw.shape, BF16),
                       jax.ShapeDtypeStruct((kv_heads, 2, 2, chunk, HEAD_DIM), BF16),
                       jax.ShapeDtypeStruct((2, 8, HEAD_DIM), F32)),
            in_specs=[any_spec] * 4 + [vmem_spec] * 4,
            out_specs=(any_spec, any_spec, vmem_spec),
            scratch_shapes=[
                pltpu.VMEM((side, 2, local_rows, per_kv, HEAD_DIM), BF16),
                pltpu.VMEM((side, 2, local_rows, per_kv, HEAD_DIM), BF16),
                pltpu.VMEM((2 * side, side, 2, 3, chunk, HEAD_DIM), BF16),
                pltpu.VMEM((side, 2, 2, per_kv, local_rows), F32),
                pltpu.VMEM((2 * side, rows, HEAD_DIM), BF16),
                pltpu.VMEM((2 * side, rows, HEAD_DIM), BF16),
                pltpu.VMEM((2 * side, HEAD_DIM, rows), BF16),
                pltpu.VMEM((2 * side, HEAD_DIM, rows), BF16),
                pltpu.VMEM((2 * side, rows, HEAD_DIM), F32),
                pltpu.VMEM((2 * side, rows, HEAD_DIM), F32),
                pltpu.VMEM((2 * side, rows, HEAD_DIM), F32),
                pltpu.VMEM((2 * side, side, 2, HEAD_DIM, 2 * chunk), F32),
                pltpu.VMEM((side, 2, side, 2, HEAD_DIM, 2 * chunk), F32),
                pltpu.VMEM((2 * side, rows, HEAD_DIM), F32),
                pltpu.VMEM((side, 2, local_rows, per_kv, HEAD_DIM), BF16),
                pltpu.VMEM((2, side, 2, 2, chunk, HEAD_DIM), BF16),
                pltpu.VMEM((8, HEAD_DIM), F32),
                pltpu.VMEM((8, HEAD_DIM), F32),
                pltpu.VMEM((3, side, 2, 8, HEAD_DIM), F32),
                dma((3, 2, side)), dma((2, 2, side)), dma((2, side, 2)), dma((side, 2)), dma((side, 2)), dma((side, 2)),
                dma((side, 2, side)), dma((side, 2, side)), dma((2 * side, side)), dma((side, 2, side)),
                dma((side, 2, 2)), dma((kv_heads, 2)), dma((2, side, 2)), dma((kv_heads, 2)),
                dma((3, side)), dma((3, side)),
            ],
            compiler_params=pltpu.CompilerParams(collective_id=0, has_side_effects=True, vmem_limit_bytes=60 << 20),
            name='attention_backward',
        )(q_raw, d_out, kv, stats, cos_t, sin_t, q_norm[None, :], k_norm[None, :])
        dkv = dkv.transpose(2, 1, 3, 0, 4).reshape(2, local_rows, kv_heads, HEAD_DIM)
        dw = jnp.sum(dw, axis=1)
        return dq_raw, dkv[0], dkv[1], dw[0], dw[1]

    row_spec = P(('dp', 'cp'))
    in_specs = (row_spec, row_spec, row_spec, row_spec, row_spec, row_spec, P(), P())
    out_specs = (row_spec, row_spec, row_spec, P('dp'), P('dp'))
    return jax.shard_map(local_grads, mesh=mesh, in_specs=in_specs, out_specs=out_specs, check_vma=False)
```

```python
import functools
import math

import jax
import jax.numpy as jnp
import numpy as np
from jax import lax
from jax.experimental import pallas as pl
from jax.experimental.pallas import tpu as pltpu
from jax.sharding import PartitionSpec as P

HEAD_DIM = 128
ROPE_THETA = 1000000.0
NORM_EPS = 1e-6
SM_SCALE = HEAD_DIM ** -0.5
LOG2E = math.log2(math.e)
F32, BF16 = jnp.float32, jnp.bfloat16
NN = (((1,), (0,)), ((), ()))
NT = (((1,), (1,)), ((), ()))


def rope_tables(positions):
    inv_freq = ROPE_THETA ** (-np.arange(0, HEAD_DIM, 2) / HEAD_DIM)
    angles = np.concatenate([positions[:, None] * inv_freq] * 2, axis=-1)
    return jnp.asarray(np.cos(angles), F32), jnp.asarray(np.sin(angles), F32)


def dot(a, b, dims):
    return lax.dot_general(a, b, dims, preferred_element_type=F32)


def kernel(side, chunk, per_kv, q_hbm, do_hbm, out_hbm, k_ref, v_ref, lse_ref, offc_ref, offs_ref, begc_ref, begs_ref, qn_ref, kn_ref,
           dq_hbm, dk_ref, dv_ref, dw_ref,
           cos_ref, sin_ref, do_v, out_v, kv_out, st_out, kst, dk_in, ld_sem,
           qbuf, dobuf, kbuf, stbuf, q_s, do_s, qT, doT, lc, dc, rb, acc, rsbuf, dq_acc, dqo, dko, dwq, dwk, xbuf,
           in_send, kv_send, kv_recv, st_recv, q_recv, do_recv, ag_send, ag_recv, rs_send, rs_recv,
           dq_send, dq_recv, dk_send, dk_recv, x_send, x_recv):
    me = lax.axis_index('cp')
    core = lax.rem(me, 2)
    chip = me // 2
    x = lax.rem(chip, side)
    y = chip // side
    a = (1 - core) * x + core * y
    b = (1 - core) * y + core * x
    head = core * side + a
    top = 2 * side - 1
    n_groups = 2 * side
    SUB = chunk
    local_rows = 2 * chunk
    rows = 2 * chunk * per_kv
    tile = side * 2 * chunk

    n_chunks = 2 * side * side

    def inv_rms(xr):
        return lax.rsqrt(jnp.mean(xr * xr, axis=-1, keepdims=True) + NORM_EPS)

    def spread(view, width):
        return jnp.concatenate([view[pl.ds(i, width, stride=0), :] for i in range(chunk)], axis=0)

    def role_dev(role, ra, rb):
        return ((1 - role) * (rb * side + ra) + role * (ra * side + rb)) * 2 + role

    def dev(d):
        return {'cp': d}

    def remote(src, dst, ssem, rsem, d):
        return pltpu.make_async_remote_copy(src_ref=src, dst_ref=dst, send_sem=ssem, recv_sem=rsem,
                                            device_id=dev(d), device_id_type=pl.DeviceIdType.MESH)

    def landed(ref, sem):
        pltpu.make_async_copy(ref, ref, sem).wait()

    loads = [pltpu.make_async_copy(do_hbm, do_v, ld_sem.at[0]), pltpu.make_async_copy(out_hbm, out_v, ld_sem.at[1])]
    for cp in loads:
        cp.start()

    barrier = pltpu.get_barrier_semaphore()
    for dx in range(side):
        for cc in range(2):
            in_row = (y * side + lax.rem(x + dx, side)) * 2 + cc
            in_col = (lax.rem(y + dx, side) * side + x) * 2 + cc
            if dx == 0:
                if cc == 0:
                    pl.semaphore_signal(barrier, inc=1, device_id=dev(chip * 2 + 1 - core), device_id_type=pl.DeviceIdType.MESH)
            else:
                pl.semaphore_signal(barrier, inc=1, device_id=dev(in_row), device_id_type=pl.DeviceIdType.MESH)
                pl.semaphore_signal(barrier, inc=1, device_id=dev(in_col), device_id_type=pl.DeviceIdType.MESH)

    def table_body(t, _):
        s, cs, lohi = t // 4, lax.rem(t // 2, 2), lax.rem(t, 2)
        src = ((1 - core) * (b * side + s) + core * (s * side + b)) * 2 + cs
        beg = src + lohi * (2 * n_chunks - 1 - 2 * src)
        bc, bs = begc_ref[pl.ds(beg, 1), :], begs_ref[pl.ds(beg, 1), :]
        oc, os = offc_ref[...], offs_ref[...]
        sign = jnp.where(lax.broadcasted_iota(jnp.int32, oc.shape, 1) < HEAD_DIM // 2, -1.0, 1.0)
        cos_ref[s, cs, lohi] = bc * oc - bs * os
        sin_ref[s, cs, lohi] = (bs * oc + bc * os) * sign
        return 0
    lax.fori_loop(0, 4 * side, table_body, 0)

    for lohi in range(2):
        part = slice(lohi * chunk, (lohi + 1) * chunk)
        kf = k_ref[part].astype(F32).reshape(chunk * n_groups, HEAD_DIM)
        nk = kf * inv_rms(kf) * kn_ref[...]
        kb = nk * spread(cos_ref.at[a, core, lohi], n_groups) + pltpu.roll(nk, HEAD_DIM // 2, 1) * spread(sin_ref.at[a, core, lohi], n_groups)
        vf = v_ref[part].astype(F32).reshape(chunk * n_groups, HEAD_DIM)
        for n, val in enumerate((kb, vf, kf)):
            kst[n] = val
            for h in range(n_groups):
                kv_out[h, lohi, n] = kst[n, pl.ds(h, chunk, stride=n_groups), :].astype(BF16)

    pl.semaphore_wait(barrier, 4 * (side - 1) + 1)

    def in_copies(role, ra, slot):
        hd = role * side + ra
        group = pl.ds(pl.multiple_of(hd * per_kv, per_kv), per_kv)
        kv = []
        for lohi in range(2):
            jj = y if lohi == 0 else top - y
            ii = x if lohi == 0 else side - 1 - x
            half = core if lohi == 0 else 1 - core
            kv.append((kv_out.at[hd, lohi], kbuf.at[jj, ii, half], kv_send.at[lohi, role, ra], kv_recv.at[lohi, slot, core]))
        return kv + [(st_out.at[hd], stbuf.at[slot, core], in_send.at[0, role, ra], st_recv.at[slot, core]),
                     (q_hbm.at[:, group, :], qbuf.at[slot, core], in_send.at[1, role, ra], q_recv.at[slot, core]),
                     (do_hbm.at[:, group, :], dobuf.at[slot, core], in_send.at[2, role, ra], do_recv.at[slot, core])]

    def coord(role):
        return x if role == 0 else y

    def targets():
        part = 1 - core
        part_a = (1 - part) * x + part * y
        yield part, part_a, part_a, chip * 2 + part
        for dx in (1, side - 1) + tuple(range(2, side - 1)):
            for role in range(2):
                ra = lax.rem(coord(role) + dx, side)
                yield role, ra, coord(role), role_dev(role, ra, y if role == 0 else x)

    own = in_copies(core, a, a)
    sends = []
    for role, ra, slot, d in targets():
        sends.append([remote(s, t, ss, rs, d) for s, t, ss, rs in in_copies(role, ra, slot)])
    def start_own(which):
        for n in which:
            pltpu.make_async_copy(own[n][0], own[n][1], own[n][3]).start()

    def start_sends(groups, which):
        for group in groups:
            for n in which:
                group[n].start()

    start_own((0, 1))
    start_sends(sends, (0, 1))
    start_own((3, 4))
    start_sends(sends[:1], (3, 4))

    acc[...] = jnp.zeros_like(acc)
    dq_acc[...] = jnp.zeros_like(dq_acc)
    dwq[...] = jnp.zeros_like(dwq)
    dwk[...] = jnp.zeros_like(dwk)

    for cp in loads:
        cp.wait()
    lane = lax.broadcasted_iota(jnp.int32, (n_groups * per_kv, local_rows), 1)

    def delta_body(t, d):
        for i in range(8):
            r = t * 8 + i
            prod = do_v[r].astype(F32) * out_v[r].astype(F32)
            d = jnp.where(lane == r, jnp.sum(prod, axis=-1, keepdims=True), d)
        return d
    delta = lax.fori_loop(0, local_rows // 8, delta_body, jnp.zeros(lane.shape, F32))
    lse2 = lse_ref[...].T * LOG2E
    for g in range(n_groups):
        st_out[g, 0] = lse2[g * per_kv:(g + 1) * per_kv]
        st_out[g, 1] = delta[g * per_kv:(g + 1) * per_kv]
    start_own((2,))
    start_sends(sends, (2,))

    def wanted(lohi, owner, user):
        return jnp.logical_or(jnp.logical_or(core == 1, lohi == 0), user <= owner)

    def place(lohi, s, bb):
        ys, xs = (1 - core) * bb + core * s, (1 - core) * s + core * bb
        return (ys, xs) if lohi == 0 else (top - ys, side - 1 - xs)

    for ds in range(side):
        s = lax.rem(a + ds, side)
        for lohi in range(2):
            jj, ii = place(lohi, s, b)
            for cc in range(2):
                landed(kbuf.at[jj, ii, cc], kv_recv.at[lohi, s, cc])
            piece = kbuf.at[jj, ii, :, pl.ds(0, 2)]
            for db in range(1, side):
                user = lax.rem(b + db, side)

                @pl.when(wanted(lohi, b, user))
                def _():
                    remote(piece, piece, ag_send.at[db, lohi, s], ag_recv.at[b, lohi, s], role_dev(core, a, user)).start()

    for ds in range(side):
        for lohi in range(2):
            for db in range(1, side):
                @pl.when(wanted(lohi, b, lax.rem(b + db, side)))
                def _():
                    landed(kbuf.at[0, 0, :, pl.ds(0, 2)], ag_send.at[db, lohi, ds])
    start_sends(sends[1:], (3, 4))

    def piece_owner(j, i):
        hi = j // side
        jj = j + hi * (top - 2 * j)
        ii = i + hi * (side - 1 - 2 * i)
        return hi, (1 - core) * jj + core * ii, (1 - core) * ii + core * jj

    def block_index(s, lohi):
        cc = (1 - core) * (b * side + s) + core * (s * side + b)
        return cc + lohi * (2 * side * side - 1 - 2 * cc)

    def stat_rows(n, s, cs, first):
        t = pltpu.roll(stbuf[s, cs, n], local_rows - first, 1)
        return jnp.concatenate([jnp.broadcast_to(t[:, i:i + 1], (per_kv, HEAD_DIM)) for i in range(SUB)], axis=0)

    def steps(fn):
        n = chunk // SUB

        def body(t, _):
            fn(t, t // n, lax.rem(t, n))
            return 0
        lax.fori_loop(0, 2 * n, body, 0)

    step_rows = SUB * per_kv

    def prepare(s, lohi):
        bi = s * 2 + lohi

        def one(t, cs, sub):
            src = pl.ds(pl.multiple_of(lohi * chunk + sub * SUB, SUB), SUB)
            dst = pl.ds(pl.multiple_of(t * step_rows, step_rows), step_rows)
            xq = qbuf[s, cs, src].astype(F32).reshape(step_rows, HEAD_DIM)
            ms = jnp.mean(xq * xq, axis=-1, keepdims=True)
            r = jnp.broadcast_to(lax.rsqrt(ms + NORM_EPS), xq.shape)
            rb[bi, dst, :] = r
            nq = xq * r * qn_ref[...]
            qf = nq * spread(cos_ref.at[s, cs, lohi], per_kv) + pltpu.roll(nq, HEAD_DIM // 2, 1) * spread(sin_ref.at[s, cs, lohi], per_kv)
            qf = qf.astype(BF16)
            q_s[bi, dst, :] = qf
            qT[bi, :, dst] = qf.T
            dof = dobuf[s, cs, src].astype(F32).reshape(step_rows, HEAD_DIM)
            dof = dof.astype(BF16)
            do_s[bi, dst, :] = dof
            doT[bi, :, dst] = dof.T
            lc[bi, dst, :] = stat_rows(0, s, cs, lohi * chunk + sub * SUB)
            dc[bi, dst, :] = stat_rows(1, s, cs, lohi * chunk + sub * SUB)
        steps(one)

    def norm_back(g, xr, r, w, cos_t, sin_t):
        dn = g * cos_t - pltpu.roll(g, HEAD_DIM // 2, 1) * sin_t
        xh = xr * r
        t = dn * w
        dx = r * (t - xh * jnp.mean(t * xh, axis=-1, keepdims=True))
        return dx, dn * xh

    def finish(s, lohi):
        bi = s * 2 + lohi

        def one(t, cs, sub):
            src = pl.ds(pl.multiple_of(lohi * chunk + sub * SUB, SUB), SUB)
            dst = pl.ds(pl.multiple_of(t * step_rows, step_rows), step_rows)
            xq = qbuf[s, cs, src].astype(F32).reshape(step_rows, HEAD_DIM)
            dx, dwt = norm_back(dq_acc[bi, dst, :] * SM_SCALE, xq, rb[bi, dst, :], qn_ref[...],
                                spread(cos_ref.at[s, cs, lohi], per_kv), spread(sin_ref.at[s, cs, lohi], per_kv))
            dwq[...] += jnp.sum(dwt.reshape(step_rows // 8, 8, HEAD_DIM), axis=0)
            dqo[s, cs, src] = dx.reshape(SUB, per_kv, HEAD_DIM).astype(BF16)
        steps(one)
        for cs in range(2):
            part = pl.ds(pl.multiple_of(lohi * chunk, chunk), chunk)
            src = dqo.at[s, cs, part]
            dst = dq_hbm.at[part, pl.ds(pl.multiple_of(head * per_kv, per_kv), per_kv), :]
            target = ((1 - core) * (b * side + s) + core * (s * side + b)) * 2 + cs
            mine = target == me

            @pl.when(mine)
            def _():
                pltpu.make_async_copy(src, dst, dq_recv.at[head, lohi]).start()

            @pl.when(jnp.logical_not(mine))
            def _():
                remote(src, dst, dq_send.at[s, cs, lohi], dq_recv.at[head, lohi], target).start()

    def compute(s, lohi, j, masked):
        bi = s * 2 + lohi
        kt = kbuf[j, :, :, 0].reshape(tile, HEAD_DIM)
        vt = kbuf[j, :, :, 1].reshape(tile, HEAD_DIM)
        z = dot(q_s[bi], kt, NT) * (SM_SCALE * LOG2E) - jnp.tile(lc[bi], (1, tile // HEAD_DIM))
        if masked:
            first = block_index(s, lohi)
            row = lax.broadcasted_iota(jnp.int32, (rows, tile), 0) // per_kv
            half, off = row // chunk, lax.rem(row, chunk)
            half = half + lohi * (1 - 2 * half)
            q_pos = first * (2 * chunk) + half * chunk + off
            k_pos = lax.broadcasted_iota(jnp.int32, (rows, tile), 1) + j * tile
            z = jnp.where(k_pos <= q_pos, z, -jnp.inf)
        p = jnp.exp2(z)
        dp = dot(do_s[bi], vt, NT)
        ds = (p * (dp - jnp.tile(dc[bi], (1, tile // HEAD_DIM)))).astype(BF16)
        pb = p.astype(BF16)
        dv_t = dot(doT[bi], pb, NN)
        dk_t = dot(qT[bi], ds, NN)
        for i in range(side):
            cols = slice(i * 2 * chunk, (i + 1) * 2 * chunk)
            acc[j, i, 0] += dk_t[:, cols]
            acc[j, i, 1] += dv_t[:, cols]
        dq_acc[bi] += dot(ds, kt, NN)

    def rs_copy(j, i, lohi, ob, os):
        return remote(acc.at[j, i], rsbuf.at[b, lohi, os], rs_send.at[j, i], rs_recv.at[b, lohi, os], role_dev(core, a, ob))

    n_group = 3

    def group_slot(grp, k):
        n = grp + k
        return lax.rem(a + n + (n // 2) * (side + 1 - 2 * n), side)

    def group_body(grp, _):
        per_group = 1 + grp // 2

        def prep_body(k, _):
            s = group_slot(grp, k)
            for cs in range(2):
                landed(stbuf.at[s, cs], st_recv.at[s, cs])
                landed(qbuf.at[s, cs], q_recv.at[s, cs])
                landed(dobuf.at[s, cs], do_recv.at[s, cs])
            prepare(s, 0)
            prepare(s, 1)
            return 0
        lax.fori_loop(0, per_group, prep_body, 0)

        def tile_body(j, _):
            @pl.when(grp == 0)
            def _():
                for i in range(side):
                    lohi, ob, os = piece_owner(j, i)

                    @pl.when(jnp.logical_and(ob != b, wanted(lohi, ob, b)))
                    def _():
                        landed(kbuf.at[j, i, :, pl.ds(0, 2)], ag_recv.at[ob, lohi, os])

            def block_body(k, _):
                s, lohi = group_slot(grp, k // 2), lax.rem(k, 2)
                full = block_index(s, lohi) // side

                @pl.when(j < full)
                def _():
                    compute(s, lohi, j, False)

                @pl.when(j == full)
                def _():
                    compute(s, lohi, j, True)
                    finish(s, lohi)
                return 0
            lax.fori_loop(0, 2 * per_group, block_body, 0)

            @pl.when(grp == n_group - 1)
            def _():
                for i in range(side):
                    lohi, ob, os = piece_owner(j, i)

                    @pl.when(jnp.logical_and(ob != b, wanted(lohi, ob, b)))
                    def _():
                        rs_copy(j, i, lohi, ob, os).start()
            return 0
        lax.fori_loop(0, 2 * side, tile_body, 0)
        return 0
    lax.fori_loop(0, n_group, group_body, 0)

    def own_body(t, _):
        lohi, s = t // side, lax.rem(t, side)
        ys, xs = (1 - core) * b + core * s, (1 - core) * s + core * b
        jj = ys + lohi * (top - 2 * ys)
        ii = xs + lohi * (side - 1 - 2 * xs)
        for db in range(1, side):
            ob = lax.rem(b + db, side)

            @pl.when(wanted(lohi, b, ob))
            def _():
                landed(rsbuf.at[ob, lohi, s], rs_recv.at[ob, lohi, s])
                acc[jj, ii] += rsbuf[ob, lohi, s]
        total = [acc[jj, ii, n] for n in range(2)]
        dk, dv = total[0].T * SM_SCALE, total[1].T
        for half in range(2):
            cs = half + lohi * (1 - 2 * half)
            part = slice(half * chunk, (half + 1) * chunk)
            kr = kbuf[jj, ii, half, 2].astype(F32)
            dx, dwt = norm_back(dk[part], kr, inv_rms(kr), kn_ref[...], cos_ref[s, cs, lohi], sin_ref[s, cs, lohi])
            dwk[...] += jnp.sum(dwt.reshape(chunk // 8, 8, HEAD_DIM), axis=0)
            dko[lohi, s, half, 0] = dx.astype(BF16)
            dko[lohi, s, half, 1] = dv[part].astype(BF16)
            target = ((1 - core) * (b * side + s) + core * (s * side + b)) * 2 + cs
            src, dst = dko.at[lohi, s, half], dk_in.at[head, lohi]
            mine = target == me

            @pl.when(mine)
            def _():
                pltpu.make_async_copy(src, dst, dk_recv.at[head, lohi]).start()

            @pl.when(jnp.logical_not(mine))
            def _():
                remote(src, dst, dk_send.at[lohi, s, half], dk_recv.at[head, lohi], target).start()
        return 0
    lax.fori_loop(0, 2 * side, own_body, 0)

    mine = x * 2 + core
    xbuf[0, mine, 0] = dwq[...]
    xbuf[0, mine, 1] = dwk[...]
    for stage, (pos, count) in enumerate(((mine, 2 * side), (y, side))):
        cps = []
        for d in range(1, count):
            o = lax.rem(pos + d, count)
            other = y * 2 * side + o if stage == 0 else (o * side + x) * 2 + core
            cp = remote(xbuf.at[stage, pos], xbuf.at[stage, pos], x_send.at[stage, d], x_recv.at[stage, pos], other)
            cp.start()
            cps.append(cp)
        for d in range(1, count):
            o = lax.rem(pos + d, count)
            landed(xbuf.at[stage, o], x_recv.at[stage, o])
        total = xbuf[stage, 0]
        for o in range(1, count):
            total = total + xbuf[stage, o]
        for cp in cps:
            cp.wait_send()
        if stage == 0:
            xbuf[1, y] = total
    dw_ref[...] = jnp.sum(total, axis=1)

    for group in sends:
        for cp in group:
            cp.wait_send()
    def drain_rs(j, _):
        for i in range(side):
            lohi, ob, os = piece_owner(j, i)

            @pl.when(jnp.logical_and(ob != b, wanted(lohi, ob, b)))
            def _():
                rs_copy(j, i, lohi, ob, os).wait_send()
        return 0
    lax.fori_loop(0, 2 * side, drain_rs, 0)

    def drain_out(t, _):
        s, lohi = t // 2, lax.rem(t, 2)
        for cs in range(2):
            target = ((1 - core) * (b * side + s) + core * (s * side + b)) * 2 + cs
            half = cs + lohi * (1 - 2 * cs)

            @pl.when(target != me)
            def _():
                part = dqo.at[s, cs, pl.ds(0, chunk)]
                pltpu.make_async_copy(part, part, dq_send.at[s, cs, lohi]).wait()
                part = dko.at[lohi, s, half]
                pltpu.make_async_copy(part, part, dk_send.at[lohi, s, half]).wait()
        return 0
    lax.fori_loop(0, 2 * side, drain_out, 0)

    def drain_in(t, _):
        hd, lohi = t // 2, lax.rem(t, 2)
        part = pl.ds(pl.multiple_of(lohi * chunk, chunk), chunk)
        landed(dq_hbm.at[part, pl.ds(pl.multiple_of(hd * per_kv, per_kv), per_kv), :], dq_recv.at[hd, lohi])
        landed(dk_in.at[hd, lohi], dk_recv.at[hd, lohi])
        return 0
    lax.fori_loop(0, 4 * side, drain_in, 0)
    for n, ref in enumerate((dk_ref, dv_ref)):
        for lohi in range(2):
            for h in range(n_groups):
                kst[n, pl.ds(h, chunk, stride=n_groups), :] = dk_in[h, lohi, n].astype(F32)
            ref[lohi * chunk:(lohi + 1) * chunk] = kst[n].reshape(chunk, n_groups, HEAD_DIM).astype(BF16)


def solution(mesh):
    cp_size = mesh.shape['cp']
    side = math.isqrt(cp_size // 2)

    def local_grads(q_raw, k_raw, v_proj, out_fwd, lse_fwd, d_out, q_norm, k_norm):
        local_rows, num_heads = q_raw.shape[0], q_raw.shape[1]
        chunk = local_rows // 2
        kv_heads = k_raw.shape[1]
        per_kv = num_heads // kv_heads
        off_cos, off_sin = rope_tables(np.arange(chunk))
        beg_cos, beg_sin = rope_tables(np.arange(2 * cp_size) * chunk)

        rows = local_rows * per_kv
        dma = pltpu.SemaphoreType.DMA
        any_spec, vmem_spec = pl.BlockSpec(memory_space=pl.ANY), pl.BlockSpec(memory_space=pltpu.VMEM)
        return pl.pallas_call(
            functools.partial(kernel, side, chunk, per_kv),
            out_shape=(jax.ShapeDtypeStruct(q_raw.shape, BF16),
                       jax.ShapeDtypeStruct(k_raw.shape, BF16),
                       jax.ShapeDtypeStruct(k_raw.shape, BF16),
                       jax.ShapeDtypeStruct((2, HEAD_DIM), F32)),
            in_specs=[any_spec] * 3 + [vmem_spec] * 9,
            out_specs=(any_spec, vmem_spec, vmem_spec, vmem_spec),
            scratch_shapes=[
                pltpu.VMEM((side, 2, 2, chunk, HEAD_DIM), F32),
                pltpu.VMEM((side, 2, 2, chunk, HEAD_DIM), F32),
                pltpu.VMEM(q_raw.shape, BF16),
                pltpu.VMEM(q_raw.shape, BF16),
                pltpu.VMEM((kv_heads, 2, 3, chunk, HEAD_DIM), BF16),
                pltpu.VMEM((kv_heads, 2, per_kv, local_rows), F32),
                pltpu.VMEM((3, chunk * kv_heads, HEAD_DIM), F32),
                pltpu.VMEM((kv_heads, 2, 2, chunk, HEAD_DIM), BF16),
                dma((2,)),
                pltpu.VMEM((side, 2, local_rows, per_kv, HEAD_DIM), BF16),
                pltpu.VMEM((side, 2, local_rows, per_kv, HEAD_DIM), BF16),
                pltpu.VMEM((2 * side, side, 2, 3, chunk, HEAD_DIM), BF16),
                pltpu.VMEM((side, 2, 2, per_kv, local_rows), F32),
                pltpu.VMEM((2 * side, rows, HEAD_DIM), BF16),
                pltpu.VMEM((2 * side, rows, HEAD_DIM), BF16),
                pltpu.VMEM((2 * side, HEAD_DIM, rows), BF16),
                pltpu.VMEM((2 * side, HEAD_DIM, rows), BF16),
                pltpu.VMEM((2 * side, rows, HEAD_DIM), F32),
                pltpu.VMEM((2 * side, rows, HEAD_DIM), F32),
                pltpu.VMEM((2 * side, rows, HEAD_DIM), F32),
                pltpu.VMEM((2 * side, side, 2, HEAD_DIM, 2 * chunk), F32),
                pltpu.VMEM((side, 2, side, 2, HEAD_DIM, 2 * chunk), F32),
                pltpu.VMEM((2 * side, rows, HEAD_DIM), F32),
                pltpu.VMEM((side, 2, local_rows, per_kv, HEAD_DIM), BF16),
                pltpu.VMEM((2, side, 2, 2, chunk, HEAD_DIM), BF16),
                pltpu.VMEM((8, HEAD_DIM), F32),
                pltpu.VMEM((8, HEAD_DIM), F32),
                pltpu.VMEM((2, 2 * side, 2, 8, HEAD_DIM), F32),
                dma((3, 2, side)), dma((2, 2, side)), dma((2, side, 2)), dma((side, 2)), dma((side, 2)), dma((side, 2)),
                dma((side, 2, side)), dma((side, 2, side)), dma((2 * side, side)), dma((side, 2, side)),
                dma((side, 2, 2)), dma((kv_heads, 2)), dma((2, side, 2)), dma((kv_heads, 2)),
                dma((2, 2 * side)), dma((2, 2 * side)),
            ],
            compiler_params=pltpu.CompilerParams(collective_id=0, has_side_effects=True, vmem_limit_bytes=63 << 20),
            name='attention_backward',
        )(q_raw, d_out, out_fwd, k_raw, v_proj, lse_fwd, off_cos, off_sin, beg_cos, beg_sin, q_norm[None, :], k_norm[None, :])

    def grads(*args):
        dq_raw, dk_raw, dv_proj, dw = local_grads(*args)
        return dq_raw, dk_raw, dv_proj, dw[0], dw[1]

    row_spec = P(('dp', 'cp'))
    in_specs = (row_spec, row_spec, row_spec, row_spec, row_spec, row_spec, P(), P())
    out_specs = (row_spec, row_spec, row_spec, P('dp'), P('dp'))
    return jax.shard_map(grads, mesh=mesh, in_specs=in_specs, out_specs=out_specs, check_vma=False)
```

```python
import functools
import math

import jax
import jax.numpy as jnp
import numpy as np
from jax import lax
from jax.experimental import pallas as pl
from jax.experimental.pallas import tpu as pltpu
from jax.sharding import PartitionSpec as P

HEAD_DIM = 128
ROPE_THETA = 1000000.0
NORM_EPS = 1e-6
SM_SCALE = HEAD_DIM ** -0.5
LOG2E = math.log2(math.e)
F32, BF16 = jnp.float32, jnp.bfloat16
NN = (((1,), (0,)), ((), ()))
NT = (((1,), (1,)), ((), ()))


def rope_tables(positions):
    inv_freq = ROPE_THETA ** (-np.arange(0, HEAD_DIM, 2) / HEAD_DIM)
    angles = np.concatenate([positions[:, None] * inv_freq] * 2, axis=-1)
    return jnp.asarray(np.cos(angles), F32), jnp.asarray(np.sin(angles), F32)


def dot(a, b, dims):
    return lax.dot_general(a, b, dims, preferred_element_type=F32)


def kernel(side, chunk, per_kv, q_hbm, do_hbm, out_hbm, k_ref, v_ref, lse_ref, offc_ref, offs_ref, begc_ref, begs_ref, qn_ref, kn_ref,
           dq_hbm, dk_ref, dv_ref, dwq_ref, dwk_ref,
           cos_ref, sin_ref, do_v, out_v, kv_out, st_out, kst, dk_in, ld_sem,
           qbuf, dobuf, kbuf, stbuf, q_s, do_s, qT, doT, lc, dc, rb, acc, rsbuf, dq_acc, dqo, dko, dwq, dwk, xbuf,
           in_send, kv_send, kv_recv, st_recv, q_recv, do_recv, ag_send, ag_recv, rs_send, rs_recv,
           dq_send, dq_recv, dk_send, dk_recv, x_send, x_recv):
    me = lax.axis_index('cp')
    core = lax.rem(me, 2)
    chip = me // 2
    x = lax.rem(chip, side)
    y = chip // side
    a = (1 - core) * x + core * y
    b = (1 - core) * y + core * x
    head = core * side + a
    top = 2 * side - 1
    n_dev = 2 * side * side
    n_groups = 2 * side
    SUB = chunk
    local_rows = 2 * chunk
    rows = 2 * chunk * per_kv
    tile = side * 2 * chunk

    n_chunks = 2 * side * side

    def inv_rms(xr):
        return lax.rsqrt(jnp.mean(xr * xr, axis=-1, keepdims=True) + NORM_EPS)

    def spread(view, width):
        return jnp.concatenate([view[pl.ds(i, width, stride=0), :] for i in range(chunk)], axis=0)

    def role_dev(role, ra, rb):
        return ((1 - role) * (rb * side + ra) + role * (ra * side + rb)) * 2 + role

    def dev(d):
        return {'cp': d}

    def remote(src, dst, ssem, rsem, d):
        return pltpu.make_async_remote_copy(src_ref=src, dst_ref=dst, send_sem=ssem, recv_sem=rsem,
                                            device_id=dev(d), device_id_type=pl.DeviceIdType.MESH)

    def landed(ref, sem):
        pltpu.make_async_copy(ref, ref, sem).wait()

    loads = [pltpu.make_async_copy(do_hbm, do_v, ld_sem.at[0]), pltpu.make_async_copy(out_hbm, out_v, ld_sem.at[1])]
    for cp in loads:
        cp.start()

    barrier = pltpu.get_barrier_semaphore()

    def greet(d, _):
        pl.semaphore_signal(barrier, inc=1, device_id=dev(lax.rem(me + d, n_dev)), device_id_type=pl.DeviceIdType.MESH)
        return 0
    lax.fori_loop(1, n_dev, greet, 0)

    def table(s, cs, lohi):
        src = ((1 - core) * (b * side + s) + core * (s * side + b)) * 2 + cs
        beg = src + lohi * (2 * n_chunks - 1 - 2 * src)
        bc, bs = begc_ref[pl.ds(beg, 1), :], begs_ref[pl.ds(beg, 1), :]
        oc, os = offc_ref[...], offs_ref[...]
        sign = jnp.where(lax.broadcasted_iota(jnp.int32, oc.shape, 1) < HEAD_DIM // 2, -1.0, 1.0)
        cos_ref[s, cs, lohi] = bc * oc - bs * os
        sin_ref[s, cs, lohi] = (bs * oc + bc * os) * sign

    def table_body(t, _):
        table(t // 4, lax.rem(t // 2, 2), lax.rem(t, 2))
        return 0

    table(a, core, 0)
    table(a, core, 1)
    pl.semaphore_wait(barrier, n_dev - 1)

    def in_copies(role, ra, slot):
        hd = role * side + ra
        group = pl.ds(pl.multiple_of(hd * per_kv, per_kv), per_kv)
        kv = []
        for lohi in range(2):
            jj = y if lohi == 0 else top - y
            ii = x if lohi == 0 else side - 1 - x
            half = core if lohi == 0 else 1 - core
            kv.append((kv_out.at[hd, lohi], kbuf.at[jj, ii, half], kv_send.at[lohi, role, ra], kv_recv.at[lohi, slot, core]))
        return kv + [(st_out.at[hd], stbuf.at[slot, core], in_send.at[0, role, ra], st_recv.at[slot, core]),
                     (q_hbm.at[:, group, :], qbuf.at[slot, core], in_send.at[1, role, ra], q_recv.at[slot, core]),
                     (do_hbm.at[:, group, :], dobuf.at[slot, core], in_send.at[2, role, ra], do_recv.at[slot, core])]

    def coord(role):
        return x if role == 0 else y

    def targets():
        part = 1 - core
        part_a = (1 - part) * x + part * y
        yield part, part_a, part_a, chip * 2 + part
        for dx in (side - 1, 1) + tuple(range(2, side - 1)):
            for role in range(2):
                ra = lax.rem(coord(role) + dx, side)
                yield role, ra, coord(role), role_dev(role, ra, y if role == 0 else x)

    own = in_copies(core, a, a)
    sends = []
    for role, ra, slot, d in targets():
        sends.append([remote(s, t, ss, rs, d) for s, t, ss, rs in in_copies(role, ra, slot)])
    def start_own(which):
        for n in which:
            pltpu.make_async_copy(own[n][0], own[n][1], own[n][3]).start()

    def start_sends(groups, which):
        for group in groups:
            for n in which:
                group[n].start()

    near = sends[:5]
    start_own((3,))
    start_sends(near[:1], (3,))

    for lohi in range(2):
        part = slice(lohi * chunk, (lohi + 1) * chunk)
        kf = k_ref[part].astype(F32).reshape(chunk * n_groups, HEAD_DIM)
        nk = kf * inv_rms(kf) * kn_ref[...]
        kb = nk * spread(cos_ref.at[a, core, lohi], n_groups) + pltpu.roll(nk, HEAD_DIM // 2, 1) * spread(sin_ref.at[a, core, lohi], n_groups)
        vf = v_ref[part].astype(F32).reshape(chunk * n_groups, HEAD_DIM)
        for n, val in enumerate((kb, vf, kf)):
            kst[n] = val
            for h in range(n_groups):
                kv_out[h, lohi, n] = kst[n, pl.ds(h, chunk, stride=n_groups), :].astype(BF16)

    start_own((0, 1))
    start_sends(sends, (0, 1))
    start_own((4,))
    start_sends(near[:1], (4,))
    lax.fori_loop(0, 4 * side, table_body, 0)

    acc[...] = jnp.zeros_like(acc)
    dq_acc[...] = jnp.zeros_like(dq_acc)
    dwq[...] = jnp.zeros_like(dwq)
    dwk[...] = jnp.zeros_like(dwk)

    for cp in loads:
        cp.wait()
    lane = lax.broadcasted_iota(jnp.int32, (n_groups * per_kv, local_rows), 1)

    def delta_body(t, d):
        for i in range(8):
            r = t * 8 + i
            prod = do_v[r].astype(F32) * out_v[r].astype(F32)
            d = jnp.where(lane == r, jnp.sum(prod, axis=-1, keepdims=True), d)
        return d
    delta = lax.fori_loop(0, local_rows // 8, delta_body, jnp.zeros(lane.shape, F32))
    lse2 = lse_ref[...] * LOG2E
    for g in range(n_groups):
        st_out[g, 0] = lse2[g * per_kv:(g + 1) * per_kv]
        st_out[g, 1] = delta[g * per_kv:(g + 1) * per_kv]
    start_own((2,))
    start_sends(sends, (2,))

    def wanted(lohi, owner, user):
        return jnp.logical_or(jnp.logical_or(core == 1, lohi == 0), user <= owner)

    def place(lohi, s, bb):
        ys, xs = (1 - core) * bb + core * s, (1 - core) * s + core * bb
        return (ys, xs) if lohi == 0 else (top - ys, side - 1 - xs)

    for lohi in range(2):
        for ds in range(side):
            s = lax.rem(a + ds, side)
            jj, ii = place(lohi, s, b)
            for cc in range(2):
                landed(kbuf.at[jj, ii, cc], kv_recv.at[lohi, s, cc])
        for db in range(side - 1, 0, -1):
            user = lax.rem(b + db, side)

            @pl.when(wanted(lohi, b, user))
            def _():
                for ds in range(side):
                    s = lax.rem(a + ds, side)
                    jj, ii = place(lohi, s, b)
                    piece = kbuf.at[jj, ii, :, pl.ds(0, 2)]
                    remote(piece, piece, ag_send.at[db, lohi, s], ag_recv.at[b, lohi, s], role_dev(core, a, user)).start()

    def late_sends():
        for ds in range(side):
            for lohi in range(2):
                for db in range(1, side):
                    @pl.when(wanted(lohi, b, lax.rem(b + db, side)))
                    def _():
                        landed(kbuf.at[0, 0, :, pl.ds(0, 2)], ag_send.at[db, lohi, ds])
        start_sends(near[1:], (3, 4))
        start_sends(sends[5:], (3, 4))

    def piece_owner(j, i):
        hi = j // side
        jj = j + hi * (top - 2 * j)
        ii = i + hi * (side - 1 - 2 * i)
        return hi, (1 - core) * jj + core * ii, (1 - core) * ii + core * jj

    def block_index(s, lohi):
        cc = (1 - core) * (b * side + s) + core * (s * side + b)
        return cc + lohi * (2 * side * side - 1 - 2 * cc)

    def stat_rows(n, s, cs, first):
        t = pltpu.roll(stbuf[s, cs, n], local_rows - first, 1)
        return jnp.concatenate([jnp.broadcast_to(t[:, i:i + 1], (per_kv, HEAD_DIM)) for i in range(SUB)], axis=0)

    def steps(fn):
        n = chunk // SUB

        def body(t, _):
            fn(t, t // n, lax.rem(t, n))
            return 0
        lax.fori_loop(0, 2 * n, body, 0)

    step_rows = SUB * per_kv

    def prepare(s, lohi):
        bi = s * 2 + lohi

        def one(t, cs, sub):
            src = pl.ds(pl.multiple_of(lohi * chunk + sub * SUB, SUB), SUB)
            dst = pl.ds(pl.multiple_of(t * step_rows, step_rows), step_rows)
            xq = qbuf[s, cs, src].astype(F32).reshape(step_rows, HEAD_DIM)
            ms = jnp.mean(xq * xq, axis=-1, keepdims=True)
            r = jnp.broadcast_to(lax.rsqrt(ms + NORM_EPS), xq.shape)
            rb[bi, dst, :] = r
            nq = xq * r * qn_ref[...]
            qf = nq * spread(cos_ref.at[s, cs, lohi], per_kv) + pltpu.roll(nq, HEAD_DIM // 2, 1) * spread(sin_ref.at[s, cs, lohi], per_kv)
            qf = qf.astype(BF16)
            q_s[bi, dst, :] = qf
            qT[bi, :, dst] = qf.T
            dof = dobuf[s, cs, src].astype(F32).reshape(step_rows, HEAD_DIM)
            dof = dof.astype(BF16)
            do_s[bi, dst, :] = dof
            doT[bi, :, dst] = dof.T
            lc[bi, dst, :] = stat_rows(0, s, cs, lohi * chunk + sub * SUB)
            dc[bi, dst, :] = stat_rows(1, s, cs, lohi * chunk + sub * SUB)
        steps(one)

    def norm_back(g, xr, r, w, cos_t, sin_t):
        dn = g * cos_t - pltpu.roll(g, HEAD_DIM // 2, 1) * sin_t
        xh = xr * r
        t = dn * w
        dx = r * (t - xh * jnp.mean(t * xh, axis=-1, keepdims=True))
        return dx, dn * xh

    def finish(s, lohi):
        bi = s * 2 + lohi

        def one(t, cs, sub):
            src = pl.ds(pl.multiple_of(lohi * chunk + sub * SUB, SUB), SUB)
            dst = pl.ds(pl.multiple_of(t * step_rows, step_rows), step_rows)
            xq = qbuf[s, cs, src].astype(F32).reshape(step_rows, HEAD_DIM)
            dx, dwt = norm_back(dq_acc[bi, dst, :] * SM_SCALE, xq, rb[bi, dst, :], qn_ref[...],
                                spread(cos_ref.at[s, cs, lohi], per_kv), spread(sin_ref.at[s, cs, lohi], per_kv))
            dwq[...] += jnp.sum(dwt.reshape(step_rows // 8, 8, HEAD_DIM), axis=0)
            dqo[s, cs, src] = dx.reshape(SUB, per_kv, HEAD_DIM).astype(BF16)
        steps(one)
        for cs in range(2):
            part = pl.ds(pl.multiple_of(lohi * chunk, chunk), chunk)
            src = dqo.at[s, cs, part]
            dst = dq_hbm.at[part, pl.ds(pl.multiple_of(head * per_kv, per_kv), per_kv), :]
            target = ((1 - core) * (b * side + s) + core * (s * side + b)) * 2 + cs
            mine = target == me

            @pl.when(mine)
            def _():
                pltpu.make_async_copy(src, dst, dq_recv.at[head, lohi]).start()

            @pl.when(jnp.logical_not(mine))
            def _():
                remote(src, dst, dq_send.at[s, cs, lohi], dq_recv.at[head, lohi], target).start()

    def compute(s, lohi, j, masked, pieces):
        bi = s * 2 + lohi
        width = pieces * 2 * chunk
        kt = kbuf[j, 0:pieces, :, 0].reshape(width, HEAD_DIM)
        vt = kbuf[j, 0:pieces, :, 1].reshape(width, HEAD_DIM)
        z = dot(q_s[bi], kt, NT) * (SM_SCALE * LOG2E) - jnp.tile(lc[bi], (1, width // HEAD_DIM))
        if masked:
            first = block_index(s, lohi)
            row = lax.broadcasted_iota(jnp.int32, (rows, width), 0) // per_kv
            half, off = row // chunk, lax.rem(row, chunk)
            half = half + lohi * (1 - 2 * half)
            q_pos = first * (2 * chunk) + half * chunk + off
            k_pos = lax.broadcasted_iota(jnp.int32, (rows, width), 1) + j * tile
            z = jnp.where(k_pos <= q_pos, z, -jnp.inf)
        p = jnp.exp2(z)
        dp = dot(do_s[bi], vt, NT)
        ds = (p * (dp - jnp.tile(dc[bi], (1, width // HEAD_DIM)))).astype(BF16)
        pb = p.astype(BF16)
        dv_t = dot(doT[bi], pb, NN)
        dk_t = dot(qT[bi], ds, NN)
        for i in range(pieces):
            cols = slice(i * 2 * chunk, (i + 1) * 2 * chunk)
            acc[j, i, 0] += dk_t[:, cols]
            acc[j, i, 1] += dv_t[:, cols]
        dq_acc[bi] += dot(ds, kt, NN)

    def rs_copy(j, i, lohi, ob, os):
        return remote(acc.at[j, i], rsbuf.at[b, lohi, os], rs_send.at[j, i], rs_recv.at[b, lohi, os], role_dev(core, a, ob))

    n_group = 3
    LATE = 3

    def group_slot(grp, k):
        n = grp + k
        return lax.rem(a + n + (n // 2) * (side + 1 - 2 * n), side)

    def group_body(grp, _):
        per_group = 1 + grp // 2

        def prep_body(k, _):
            s = group_slot(grp, k)
            for cs in range(2):
                landed(stbuf.at[s, cs], st_recv.at[s, cs])
                landed(qbuf.at[s, cs], q_recv.at[s, cs])
                landed(dobuf.at[s, cs], do_recv.at[s, cs])
            prepare(s, 0)
            prepare(s, 1)
            return 0
        lax.fori_loop(0, per_group, prep_body, 0)

        def tile_body(t, _):
            lohi_t, n = t // side, lax.rem(t, side)
            o = lax.rem(b + n + grp // 2, side)
            j = o + lohi_t * (top - 2 * o)

            @pl.when(grp == 0)
            def _():
                @pl.when(t == LATE)
                def _():
                    late_sends()

                for i in range(side):
                    lohi, ob, os = piece_owner(j, i)

                    @pl.when(jnp.logical_and(ob != b, wanted(lohi, ob, b)))
                    def _():
                        landed(kbuf.at[j, i, :, pl.ds(0, 2)], ag_recv.at[ob, lohi, os])

            def block_body(k, _):
                s, lohi = group_slot(grp, k // 2), lax.rem(k, 2)
                index = block_index(s, lohi)
                full, wide = index // side, lax.rem(index, side) >= side // 2

                @pl.when(j < full)
                def _():
                    compute(s, lohi, j, False, side)

                @pl.when(jnp.logical_and(j == full, wide))
                def _():
                    compute(s, lohi, j, True, side)

                @pl.when(jnp.logical_and(j == full, jnp.logical_not(wide)))
                def _():
                    compute(s, lohi, j, True, side // 2)
                return 0
            lax.fori_loop(0, 2 * per_group, block_body, 0)

            @pl.when(grp == n_group - 1)
            def _():
                for i in range(side):
                    lohi, ob, os = piece_owner(j, i)

                    @pl.when(jnp.logical_and(ob != b, wanted(lohi, ob, b)))
                    def _():
                        rs_copy(j, i, lohi, ob, os).start()

            @pl.when(n == side - 1)
            def _():
                def finish_body(k, _):
                    finish(group_slot(grp, k), lohi_t)
                    return 0
                lax.fori_loop(0, per_group, finish_body, 0)
            return 0
        lax.fori_loop(0, 2 * side, tile_body, 0)
        return 0
    lax.fori_loop(0, n_group, group_body, 0)

    def own_body(t, _):
        lohi, s = t // side, lax.rem(t, side)
        ys, xs = (1 - core) * b + core * s, (1 - core) * s + core * b
        jj = ys + lohi * (top - 2 * ys)
        ii = xs + lohi * (side - 1 - 2 * xs)
        for db in range(1, side):
            ob = lax.rem(b + db, side)

            @pl.when(wanted(lohi, b, ob))
            def _():
                landed(rsbuf.at[ob, lohi, s], rs_recv.at[ob, lohi, s])
                acc[jj, ii] += rsbuf[ob, lohi, s]
        total = [acc[jj, ii, n] for n in range(2)]
        dk, dv = total[0].T * SM_SCALE, total[1].T
        for half in range(2):
            cs = half + lohi * (1 - 2 * half)
            part = slice(half * chunk, (half + 1) * chunk)
            kr = kbuf[jj, ii, half, 2].astype(F32)
            dx, dwt = norm_back(dk[part], kr, inv_rms(kr), kn_ref[...], cos_ref[s, cs, lohi], sin_ref[s, cs, lohi])
            dwk[...] += jnp.sum(dwt.reshape(chunk // 8, 8, HEAD_DIM), axis=0)
            dko[lohi, s, half, 0] = dx.astype(BF16)
            dko[lohi, s, half, 1] = dv[part].astype(BF16)
            target = ((1 - core) * (b * side + s) + core * (s * side + b)) * 2 + cs
            src, dst = dko.at[lohi, s, half], dk_in.at[head, lohi]
            mine = target == me

            @pl.when(mine)
            def _():
                pltpu.make_async_copy(src, dst, dk_recv.at[head, lohi]).start()

            @pl.when(jnp.logical_not(mine))
            def _():
                remote(src, dst, dk_send.at[lohi, s, half], dk_recv.at[head, lohi], target).start()
        return 0
    lax.fori_loop(0, 2 * side, own_body, 0)

    xbuf[me, 0] = jnp.sum(dwq[...], axis=0, keepdims=True)
    xbuf[me, 1] = jnp.sum(dwk[...], axis=0, keepdims=True)

    def x_copy(d):
        return remote(xbuf.at[me], xbuf.at[me], x_send.at[d], x_recv.at[me], lax.rem(me + d, n_dev))

    def x_start(d, _):
        x_copy(d).start()
        return 0
    lax.fori_loop(1, n_dev, x_start, 0)

    for group in sends:
        for cp in group:
            cp.wait_send()
    def drain_rs(j, _):
        for i in range(side):
            lohi, ob, os = piece_owner(j, i)

            @pl.when(jnp.logical_and(ob != b, wanted(lohi, ob, b)))
            def _():
                rs_copy(j, i, lohi, ob, os).wait_send()
        return 0
    lax.fori_loop(0, 2 * side, drain_rs, 0)

    def drain_out(t, _):
        s, lohi = t // 2, lax.rem(t, 2)
        for cs in range(2):
            target = ((1 - core) * (b * side + s) + core * (s * side + b)) * 2 + cs
            half = cs + lohi * (1 - 2 * cs)

            @pl.when(target != me)
            def _():
                part = dqo.at[s, cs, pl.ds(0, chunk)]
                pltpu.make_async_copy(part, part, dq_send.at[s, cs, lohi]).wait()
                part = dko.at[lohi, s, half]
                pltpu.make_async_copy(part, part, dk_send.at[lohi, s, half]).wait()
        return 0
    lax.fori_loop(0, 2 * side, drain_out, 0)

    def drain_in(t, _):
        hd, lohi = t // 2, lax.rem(t, 2)
        part = pl.ds(pl.multiple_of(lohi * chunk, chunk), chunk)
        landed(dq_hbm.at[part, pl.ds(pl.multiple_of(hd * per_kv, per_kv), per_kv), :], dq_recv.at[hd, lohi])
        landed(dk_in.at[hd, lohi], dk_recv.at[hd, lohi])
        return 0
    lax.fori_loop(0, 4 * side, drain_in, 0)
    def x_wait(d, _):
        x_copy(d).wait_send()
        o = lax.rem(me + d, n_dev)
        landed(xbuf.at[o], x_recv.at[o])
        return 0
    lax.fori_loop(1, n_dev, x_wait, 0)
    dwq_ref[...] = jnp.sum(xbuf[:, 0, :, :], axis=0)
    dwk_ref[...] = jnp.sum(xbuf[:, 1, :, :], axis=0)
    for n, ref in enumerate((dk_ref, dv_ref)):
        for lohi in range(2):
            for h in range(n_groups):
                kst[n, pl.ds(h, chunk, stride=n_groups), :] = dk_in[h, lohi, n].astype(F32)
            ref[lohi * chunk:(lohi + 1) * chunk] = kst[n].reshape(chunk, n_groups, HEAD_DIM).astype(BF16)


def solution(mesh):
    cp_size = mesh.shape['cp']
    side = math.isqrt(cp_size // 2)

    def local_grads(q_raw, k_raw, v_proj, out_fwd, lse_fwd, d_out, q_norm, k_norm):
        local_rows, num_heads = q_raw.shape[0], q_raw.shape[1]
        chunk = local_rows // 2
        kv_heads = k_raw.shape[1]
        per_kv = num_heads // kv_heads
        off_cos, off_sin = rope_tables(np.arange(chunk))
        beg_cos, beg_sin = rope_tables(np.arange(2 * cp_size) * chunk)

        rows = local_rows * per_kv
        dma = pltpu.SemaphoreType.DMA
        any_spec, vmem_spec = pl.BlockSpec(memory_space=pl.ANY), pl.BlockSpec(memory_space=pltpu.VMEM)
        return pl.pallas_call(
            functools.partial(kernel, side, chunk, per_kv),
            out_shape=(jax.ShapeDtypeStruct(q_raw.shape, BF16),
                       jax.ShapeDtypeStruct(k_raw.shape, BF16),
                       jax.ShapeDtypeStruct(k_raw.shape, BF16),
                       jax.ShapeDtypeStruct((1, HEAD_DIM), F32),
                       jax.ShapeDtypeStruct((1, HEAD_DIM), F32)),
            in_specs=[any_spec] * 3 + [vmem_spec] * 9,
            out_specs=(any_spec, vmem_spec, vmem_spec, vmem_spec, vmem_spec),
            scratch_shapes=[
                pltpu.VMEM((side, 2, 2, chunk, HEAD_DIM), F32),
                pltpu.VMEM((side, 2, 2, chunk, HEAD_DIM), F32),
                pltpu.VMEM(q_raw.shape, BF16),
                pltpu.VMEM(q_raw.shape, BF16),
                pltpu.VMEM((kv_heads, 2, 3, chunk, HEAD_DIM), BF16),
                pltpu.VMEM((kv_heads, 2, per_kv, local_rows), F32),
                pltpu.VMEM((3, chunk * kv_heads, HEAD_DIM), F32),
                pltpu.VMEM((kv_heads, 2, 2, chunk, HEAD_DIM), BF16),
                dma((2,)),
                pltpu.VMEM((side, 2, local_rows, per_kv, HEAD_DIM), BF16),
                pltpu.VMEM((side, 2, local_rows, per_kv, HEAD_DIM), BF16),
                pltpu.VMEM((2 * side, side, 2, 3, chunk, HEAD_DIM), BF16),
                pltpu.VMEM((side, 2, 2, per_kv, local_rows), F32),
                pltpu.VMEM((2 * side, rows, HEAD_DIM), BF16),
                pltpu.VMEM((2 * side, rows, HEAD_DIM), BF16),
                pltpu.VMEM((2 * side, HEAD_DIM, rows), BF16),
                pltpu.VMEM((2 * side, HEAD_DIM, rows), BF16),
                pltpu.VMEM((2 * side, rows, HEAD_DIM), F32),
                pltpu.VMEM((2 * side, rows, HEAD_DIM), F32),
                pltpu.VMEM((2 * side, rows, HEAD_DIM), F32),
                pltpu.VMEM((2 * side, side, 2, HEAD_DIM, 2 * chunk), F32),
                pltpu.VMEM((side, 2, side, 2, HEAD_DIM, 2 * chunk), F32),
                pltpu.VMEM((2 * side, rows, HEAD_DIM), F32),
                pltpu.VMEM((side, 2, local_rows, per_kv, HEAD_DIM), BF16),
                pltpu.VMEM((2, side, 2, 2, chunk, HEAD_DIM), BF16),
                pltpu.VMEM((8, HEAD_DIM), F32),
                pltpu.VMEM((8, HEAD_DIM), F32),
                pltpu.VMEM((cp_size, 2, 1, HEAD_DIM), F32),
                dma((3, 2, side)), dma((2, 2, side)), dma((2, side, 2)), dma((side, 2)), dma((side, 2)), dma((side, 2)),
                dma((side, 2, side)), dma((side, 2, side)), dma((2 * side, side)), dma((side, 2, side)),
                dma((side, 2, 2)), dma((kv_heads, 2)), dma((2, side, 2)), dma((kv_heads, 2)),
                dma((cp_size,)), dma((cp_size,)),
            ],
            compiler_params=pltpu.CompilerParams(collective_id=0, has_side_effects=True, vmem_limit_bytes=63 << 20),
            name='attention_backward',
        )(q_raw, d_out, out_fwd, k_raw, v_proj, lse_fwd.T, off_cos, off_sin, beg_cos, beg_sin, q_norm[None, :], k_norm[None, :])

    def grads(*args):
        dq_raw, dk_raw, dv_proj, dq_norm, dk_norm = local_grads(*args)
        return dq_raw, dk_raw, dv_proj, dq_norm[0], dk_norm[0]

    row_spec = P(('dp', 'cp'))
    in_specs = (row_spec, row_spec, row_spec, row_spec, row_spec, row_spec, P(), P())
    out_specs = (row_spec, row_spec, row_spec, P('dp'), P('dp'))
    return jax.shard_map(grads, mesh=mesh, in_specs=in_specs, out_specs=out_specs, check_vma=False)
```

```python
import functools
import math

import jax
import jax.numpy as jnp
import numpy as np
from jax import lax
from jax.experimental import pallas as pl
from jax.experimental.pallas import tpu as pltpu
from jax.sharding import PartitionSpec as P

HEAD_DIM = 128
ROPE_THETA = 1000000.0
NORM_EPS = 1e-6
SM_SCALE = HEAD_DIM ** -0.5
LOG2E = math.log2(math.e)
F32, BF16 = jnp.float32, jnp.bfloat16
NN = (((1,), (0,)), ((), ()))
NT = (((1,), (1,)), ((), ()))


def rope_tables(positions):
    inv_freq = ROPE_THETA ** (-np.arange(0, HEAD_DIM, 2) / HEAD_DIM)
    angles = np.concatenate([positions[:, None] * inv_freq] * 2, axis=-1)
    return jnp.asarray(np.cos(angles), F32), jnp.asarray(np.sin(angles), F32)


def dot(a, b, dims):
    return lax.dot_general(a, b, dims, preferred_element_type=F32)


def kernel(side, chunk, per_kv, q_hbm, do_hbm, out_hbm, k_ref, v_ref, lse_ref, offc_ref, offs_ref, begc_ref, begs_ref, qn_ref, kn_ref,
           dq_hbm, dk_ref, dv_ref, dwq_ref, dwk_ref,
           cos_ref, sin_ref, do_v, out_v, kv_out, st_out, kst, dk_in, ld_sem,
           qbuf, dobuf, kbuf, stbuf, q_s, do_s, qT, doT, lc, dc, rb, acc, rsbuf, dq_acc, dqo, dko, dwq, dwk, xbuf,
           in_send, kv_send, kv_recv, st_recv, q_recv, do_recv, ag_send, ag_recv, rs_send, rs_recv,
           dq_send, dq_recv, dk_send, dk_recv, x_send, x_recv):
    me = lax.axis_index('cp')
    core = lax.rem(me, 2)
    chip = me // 2
    x = lax.rem(chip, side)
    y = chip // side
    a = (1 - core) * x + core * y
    b = (1 - core) * y + core * x
    head = core * side + a
    top = 2 * side - 1
    n_dev = 2 * side * side
    n_groups = 2 * side
    SUB = chunk
    local_rows = 2 * chunk
    rows = 2 * chunk * per_kv
    tile = side * 2 * chunk

    n_chunks = 2 * side * side

    def inv_rms(xr):
        return lax.rsqrt(jnp.mean(xr * xr, axis=-1, keepdims=True) + NORM_EPS)

    def spread(view, width):
        return jnp.concatenate([view[pl.ds(i, width, stride=0), :] for i in range(chunk)], axis=0)

    def role_dev(role, ra, rb):
        return ((1 - role) * (rb * side + ra) + role * (ra * side + rb)) * 2 + role

    def dev(d):
        return {'cp': d}

    def remote(src, dst, ssem, rsem, d):
        return pltpu.make_async_remote_copy(src_ref=src, dst_ref=dst, send_sem=ssem, recv_sem=rsem,
                                            device_id=dev(d), device_id_type=pl.DeviceIdType.MESH)

    def landed(ref, sem):
        pltpu.make_async_copy(ref, ref, sem).wait()

    loads = [pltpu.make_async_copy(do_hbm, do_v, ld_sem.at[0]), pltpu.make_async_copy(out_hbm, out_v, ld_sem.at[1])]
    for cp in loads:
        cp.start()

    barrier = pltpu.get_barrier_semaphore()

    def greet(d, _):
        pl.semaphore_signal(barrier, inc=1, device_id=dev(lax.rem(me + d, n_dev)), device_id_type=pl.DeviceIdType.MESH)
        return 0
    lax.fori_loop(1, n_dev, greet, 0)

    def table(s, cs, lohi):
        src = ((1 - core) * (b * side + s) + core * (s * side + b)) * 2 + cs
        beg = src + lohi * (2 * n_chunks - 1 - 2 * src)
        bc, bs = begc_ref[pl.ds(beg, 1), :], begs_ref[pl.ds(beg, 1), :]
        oc, os = offc_ref[...], offs_ref[...]
        sign = jnp.where(lax.broadcasted_iota(jnp.int32, oc.shape, 1) < HEAD_DIM // 2, -1.0, 1.0)
        cos_ref[s, cs, lohi] = bc * oc - bs * os
        sin_ref[s, cs, lohi] = (bs * oc + bc * os) * sign

    def table_body(t, _):
        table(t // 4, lax.rem(t // 2, 2), lax.rem(t, 2))
        return 0

    table(a, core, 0)
    table(a, core, 1)
    pl.semaphore_wait(barrier, n_dev - 1)

    def in_copies(role, ra, slot):
        hd = role * side + ra
        group = pl.ds(pl.multiple_of(hd * per_kv, per_kv), per_kv)
        kv = []
        for lohi in range(2):
            jj = y if lohi == 0 else top - y
            ii = x if lohi == 0 else side - 1 - x
            half = core if lohi == 0 else 1 - core
            kv.append((kv_out.at[hd, lohi], kbuf.at[jj, ii, half], kv_send.at[lohi, role, ra], kv_recv.at[lohi, slot, core]))
        return kv + [(st_out.at[hd], stbuf.at[slot, core], in_send.at[0, role, ra], st_recv.at[slot, core]),
                     (q_hbm.at[:, group, :], qbuf.at[slot, core], in_send.at[1, role, ra], q_recv.at[slot, core]),
                     (do_hbm.at[:, group, :], dobuf.at[slot, core], in_send.at[2, role, ra], do_recv.at[slot, core])]

    def coord(role):
        return x if role == 0 else y

    def targets():
        part = 1 - core
        part_a = (1 - part) * x + part * y
        yield part, part_a, part_a, chip * 2 + part
        for dx in (side - 1, 1) + tuple(range(2, side - 1)):
            for role in range(2):
                ra = lax.rem(coord(role) + dx, side)
                yield role, ra, coord(role), role_dev(role, ra, y if role == 0 else x)

    own = in_copies(core, a, a)
    sends = []
    for role, ra, slot, d in targets():
        sends.append([remote(s, t, ss, rs, d) for s, t, ss, rs in in_copies(role, ra, slot)])
    def start_own(which):
        for n in which:
            pltpu.make_async_copy(own[n][0], own[n][1], own[n][3]).start()

    def start_sends(groups, which):
        for group in groups:
            for n in which:
                group[n].start()

    near = sends[:5]
    start_own((3,))
    start_sends(near, (3,))

    for lohi in range(2):
        part = slice(lohi * chunk, (lohi + 1) * chunk)
        kf = k_ref[part].astype(F32).reshape(chunk * n_groups, HEAD_DIM)
        nk = kf * inv_rms(kf) * kn_ref[...]
        kb = nk * spread(cos_ref.at[a, core, lohi], n_groups) + pltpu.roll(nk, HEAD_DIM // 2, 1) * spread(sin_ref.at[a, core, lohi], n_groups)
        vf = v_ref[part].astype(F32).reshape(chunk * n_groups, HEAD_DIM)
        for n, val in enumerate((kb, vf, kf)):
            kst[n] = val
            for h in range(n_groups):
                kv_out[h, lohi, n] = kst[n, pl.ds(h, chunk, stride=n_groups), :].astype(BF16)

    start_own((0, 1))
    start_sends(sends, (0, 1))
    start_own((4,))
    start_sends(near, (4,))
    lax.fori_loop(0, 4 * side, table_body, 0)

    acc[...] = jnp.zeros_like(acc)
    dq_acc[...] = jnp.zeros_like(dq_acc)
    dwq[...] = jnp.zeros_like(dwq)
    dwk[...] = jnp.zeros_like(dwk)

    for cp in loads:
        cp.wait()
    lane = lax.broadcasted_iota(jnp.int32, (n_groups * per_kv, local_rows), 1)

    def delta_body(t, d):
        for i in range(8):
            r = t * 8 + i
            prod = do_v[r].astype(F32) * out_v[r].astype(F32)
            d = jnp.where(lane == r, jnp.sum(prod, axis=-1, keepdims=True), d)
        return d
    delta = lax.fori_loop(0, local_rows // 8, delta_body, jnp.zeros(lane.shape, F32))
    lse2 = lse_ref[...] * LOG2E
    for g in range(n_groups):
        st_out[g, 0] = lse2[g * per_kv:(g + 1) * per_kv]
        st_out[g, 1] = delta[g * per_kv:(g + 1) * per_kv]
    start_own((2,))
    start_sends(sends, (2,))

    def wanted(lohi, owner, user):
        return jnp.logical_or(jnp.logical_or(core == 1, lohi == 0), user <= owner)

    def place(lohi, s, bb):
        ys, xs = (1 - core) * bb + core * s, (1 - core) * s + core * bb
        return (ys, xs) if lohi == 0 else (top - ys, side - 1 - xs)

    for lohi in range(2):
        for ds in range(side):
            s = lax.rem(a + ds, side)
            jj, ii = place(lohi, s, b)
            for cc in range(2):
                landed(kbuf.at[jj, ii, cc], kv_recv.at[lohi, s, cc])
        for db in range(side - 1, 0, -1):
            user = lax.rem(b + db, side)

            @pl.when(wanted(lohi, b, user))
            def _():
                for ds in range(side):
                    s = lax.rem(a + ds, side)
                    jj, ii = place(lohi, s, b)
                    piece = kbuf.at[jj, ii, :, pl.ds(0, 2)]
                    remote(piece, piece, ag_send.at[db, lohi, s], ag_recv.at[b, lohi, s], role_dev(core, a, user)).start()

    def late_sends():
        for ds in range(side):
            for lohi in range(2):
                for db in range(1, side):
                    @pl.when(wanted(lohi, b, lax.rem(b + db, side)))
                    def _():
                        landed(kbuf.at[0, 0, :, pl.ds(0, 2)], ag_send.at[db, lohi, ds])
        start_sends(sends[5:], (3, 4))

    def piece_owner(j, i):
        hi = j // side
        jj = j + hi * (top - 2 * j)
        ii = i + hi * (side - 1 - 2 * i)
        return hi, (1 - core) * jj + core * ii, (1 - core) * ii + core * jj

    def block_index(s, lohi):
        cc = (1 - core) * (b * side + s) + core * (s * side + b)
        return cc + lohi * (2 * side * side - 1 - 2 * cc)

    def stat_rows(n, s, cs, first):
        t = pltpu.roll(stbuf[s, cs, n], local_rows - first, 1)
        return jnp.concatenate([jnp.broadcast_to(t[:, i:i + 1], (per_kv, HEAD_DIM)) for i in range(SUB)], axis=0)

    def steps(fn):
        n = chunk // SUB

        def body(t, _):
            fn(t, t // n, lax.rem(t, n))
            return 0
        lax.fori_loop(0, 2 * n, body, 0)

    step_rows = SUB * per_kv

    def prepare(s, lohi):
        bi = s * 2 + lohi

        def one(t, cs, sub):
            src = pl.ds(pl.multiple_of(lohi * chunk + sub * SUB, SUB), SUB)
            dst = pl.ds(pl.multiple_of(t * step_rows, step_rows), step_rows)
            xq = qbuf[s, cs, src].astype(F32).reshape(step_rows, HEAD_DIM)
            ms = jnp.mean(xq * xq, axis=-1, keepdims=True)
            r = jnp.broadcast_to(lax.rsqrt(ms + NORM_EPS), xq.shape)
            rb[bi, dst, :] = r
            nq = xq * r * qn_ref[...]
            qf = nq * spread(cos_ref.at[s, cs, lohi], per_kv) + pltpu.roll(nq, HEAD_DIM // 2, 1) * spread(sin_ref.at[s, cs, lohi], per_kv)
            qf = qf.astype(BF16)
            q_s[bi, dst, :] = qf
            qT[bi, :, dst] = qf.T
            dof = dobuf[s, cs, src].astype(F32).reshape(step_rows, HEAD_DIM)
            dof = dof.astype(BF16)
            do_s[bi, dst, :] = dof
            doT[bi, :, dst] = dof.T
            lc[bi, dst, :] = stat_rows(0, s, cs, lohi * chunk + sub * SUB)
            dc[bi, dst, :] = stat_rows(1, s, cs, lohi * chunk + sub * SUB)
        steps(one)

    def norm_back(g, xr, r, w, cos_t, sin_t):
        dn = g * cos_t - pltpu.roll(g, HEAD_DIM // 2, 1) * sin_t
        xh = xr * r
        t = dn * w
        dx = r * (t - xh * jnp.mean(t * xh, axis=-1, keepdims=True))
        return dx, dn * xh

    def finish(s, lohi):
        bi = s * 2 + lohi

        def one(t, cs, sub):
            src = pl.ds(pl.multiple_of(lohi * chunk + sub * SUB, SUB), SUB)
            dst = pl.ds(pl.multiple_of(t * step_rows, step_rows), step_rows)
            xq = qbuf[s, cs, src].astype(F32).reshape(step_rows, HEAD_DIM)
            dx, dwt = norm_back(dq_acc[bi, dst, :] * SM_SCALE, xq, rb[bi, dst, :], qn_ref[...],
                                spread(cos_ref.at[s, cs, lohi], per_kv), spread(sin_ref.at[s, cs, lohi], per_kv))
            dwq[...] += jnp.sum(dwt.reshape(step_rows // 8, 8, HEAD_DIM), axis=0)
            dqo[s, cs, src] = dx.reshape(SUB, per_kv, HEAD_DIM).astype(BF16)
        steps(one)
        for cs in range(2):
            part = pl.ds(pl.multiple_of(lohi * chunk, chunk), chunk)
            src = dqo.at[s, cs, part]
            dst = dq_hbm.at[part, pl.ds(pl.multiple_of(head * per_kv, per_kv), per_kv), :]
            target = ((1 - core) * (b * side + s) + core * (s * side + b)) * 2 + cs
            mine = target == me

            @pl.when(mine)
            def _():
                pltpu.make_async_copy(src, dst, dq_recv.at[head, lohi]).start()

            @pl.when(jnp.logical_not(mine))
            def _():
                remote(src, dst, dq_send.at[s, cs, lohi], dq_recv.at[head, lohi], target).start()

    def compute(s, lohi, j, masked, pieces):
        bi = s * 2 + lohi
        width = pieces * 2 * chunk
        kt = kbuf[j, 0:pieces, :, 0].reshape(width, HEAD_DIM)
        vt = kbuf[j, 0:pieces, :, 1].reshape(width, HEAD_DIM)
        z = dot(q_s[bi], kt, NT) * (SM_SCALE * LOG2E) - jnp.tile(lc[bi], (1, width // HEAD_DIM))
        if masked:
            first = block_index(s, lohi)
            row = lax.broadcasted_iota(jnp.int32, (rows, width), 0) // per_kv
            half, off = row // chunk, lax.rem(row, chunk)
            half = half + lohi * (1 - 2 * half)
            q_pos = first * (2 * chunk) + half * chunk + off
            k_pos = lax.broadcasted_iota(jnp.int32, (rows, width), 1) + j * tile
            z = jnp.where(k_pos <= q_pos, z, -jnp.inf)
        p = jnp.exp2(z)
        dp = dot(do_s[bi], vt, NT)
        ds = (p * (dp - jnp.tile(dc[bi], (1, width // HEAD_DIM)))).astype(BF16)
        pb = p.astype(BF16)
        dv_t = dot(doT[bi], pb, NN)
        dk_t = dot(qT[bi], ds, NN)
        for i in range(pieces):
            cols = slice(i * 2 * chunk, (i + 1) * 2 * chunk)
            acc[j, i, 0] += dk_t[:, cols]
            acc[j, i, 1] += dv_t[:, cols]
        dq_acc[bi] += dot(ds, kt, NN)

    def rs_copy(j, i, lohi, ob, os):
        return remote(acc.at[j, i], rsbuf.at[b, lohi, os], rs_send.at[j, i], rs_recv.at[b, lohi, os], role_dev(core, a, ob))

    n_group = 3
    LATE = 3

    def group_slot(grp, k):
        n = grp + k
        return lax.rem(a + lax.rem(2 * n + 1, side + 1), side)

    def group_body(grp, _):
        per_group = 1 + grp // 2

        def prep_body(k, _):
            s = group_slot(grp, k)
            for cs in range(2):
                landed(stbuf.at[s, cs], st_recv.at[s, cs])
                landed(qbuf.at[s, cs], q_recv.at[s, cs])
                landed(dobuf.at[s, cs], do_recv.at[s, cs])
            prepare(s, 0)
            prepare(s, 1)
            return 0
        lax.fori_loop(0, per_group, prep_body, 0)

        def tile_body(t, _):
            lohi_t, n = t // side, lax.rem(t, side)
            o = lax.rem(b + n + grp // 2, side)
            j = o + lohi_t * (top - 2 * o)

            @pl.when(grp == 0)
            def _():
                @pl.when(t == LATE)
                def _():
                    late_sends()

                for i in range(side):
                    lohi, ob, os = piece_owner(j, i)

                    @pl.when(jnp.logical_and(ob != b, wanted(lohi, ob, b)))
                    def _():
                        landed(kbuf.at[j, i, :, pl.ds(0, 2)], ag_recv.at[ob, lohi, os])

            def block_body(k, _):
                s, lohi = group_slot(grp, k // 2), lax.rem(k, 2)
                index = block_index(s, lohi)
                full, wide = index // side, lax.rem(index, side) >= side // 2

                @pl.when(j < full)
                def _():
                    compute(s, lohi, j, False, side)

                @pl.when(jnp.logical_and(j == full, wide))
                def _():
                    compute(s, lohi, j, True, side)

                @pl.when(jnp.logical_and(j == full, jnp.logical_not(wide)))
                def _():
                    compute(s, lohi, j, True, side // 2)
                return 0
            lax.fori_loop(0, 2 * per_group, block_body, 0)

            @pl.when(grp == n_group - 1)
            def _():
                for i in range(side):
                    lohi, ob, os = piece_owner(j, i)

                    @pl.when(jnp.logical_and(ob != b, wanted(lohi, ob, b)))
                    def _():
                        rs_copy(j, i, lohi, ob, os).start()

            @pl.when(n == side - 1)
            def _():
                def finish_body(k, _):
                    finish(group_slot(grp, k), lohi_t)
                    return 0
                lax.fori_loop(0, per_group, finish_body, 0)
            return 0
        lax.fori_loop(0, 2 * side, tile_body, 0)
        return 0
    lax.fori_loop(0, n_group, group_body, 0)

    def own_body(t, _):
        lohi, s = t // side, lax.rem(t, side)
        ys, xs = (1 - core) * b + core * s, (1 - core) * s + core * b
        jj = ys + lohi * (top - 2 * ys)
        ii = xs + lohi * (side - 1 - 2 * xs)
        for db in range(1, side):
            ob = lax.rem(b + db, side)

            @pl.when(wanted(lohi, b, ob))
            def _():
                landed(rsbuf.at[ob, lohi, s], rs_recv.at[ob, lohi, s])
                acc[jj, ii] += rsbuf[ob, lohi, s]
        total = [acc[jj, ii, n] for n in range(2)]
        dk, dv = total[0].T * SM_SCALE, total[1].T
        for half in range(2):
            cs = half + lohi * (1 - 2 * half)
            part = slice(half * chunk, (half + 1) * chunk)
            kr = kbuf[jj, ii, half, 2].astype(F32)
            dx, dwt = norm_back(dk[part], kr, inv_rms(kr), kn_ref[...], cos_ref[s, cs, lohi], sin_ref[s, cs, lohi])
            dwk[...] += jnp.sum(dwt.reshape(chunk // 8, 8, HEAD_DIM), axis=0)
            dko[lohi, s, half, 0] = dx.astype(BF16)
            dko[lohi, s, half, 1] = dv[part].astype(BF16)
            target = ((1 - core) * (b * side + s) + core * (s * side + b)) * 2 + cs
            src, dst = dko.at[lohi, s, half], dk_in.at[head, lohi]
            mine = target == me

            @pl.when(mine)
            def _():
                pltpu.make_async_copy(src, dst, dk_recv.at[head, lohi]).start()

            @pl.when(jnp.logical_not(mine))
            def _():
                remote(src, dst, dk_send.at[lohi, s, half], dk_recv.at[head, lohi], target).start()
        return 0
    lax.fori_loop(0, 2 * side, own_body, 0)

    xbuf[me, 0] = jnp.sum(dwq[...], axis=0, keepdims=True)
    xbuf[me, 1] = jnp.sum(dwk[...], axis=0, keepdims=True)

    def x_copy(d):
        return remote(xbuf.at[me], xbuf.at[me], x_send.at[d], x_recv.at[me], lax.rem(me + d, n_dev))

    def x_start(d, _):
        x_copy(d).start()
        return 0
    lax.fori_loop(1, n_dev, x_start, 0)

    for group in sends:
        for cp in group:
            cp.wait_send()
    def drain_rs(j, _):
        for i in range(side):
            lohi, ob, os = piece_owner(j, i)

            @pl.when(jnp.logical_and(ob != b, wanted(lohi, ob, b)))
            def _():
                rs_copy(j, i, lohi, ob, os).wait_send()
        return 0
    lax.fori_loop(0, 2 * side, drain_rs, 0)

    def drain_out(t, _):
        s, lohi = t // 2, lax.rem(t, 2)
        for cs in range(2):
            target = ((1 - core) * (b * side + s) + core * (s * side + b)) * 2 + cs
            half = cs + lohi * (1 - 2 * cs)

            @pl.when(target != me)
            def _():
                part = dqo.at[s, cs, pl.ds(0, chunk)]
                pltpu.make_async_copy(part, part, dq_send.at[s, cs, lohi]).wait()
                part = dko.at[lohi, s, half]
                pltpu.make_async_copy(part, part, dk_send.at[lohi, s, half]).wait()
        return 0
    lax.fori_loop(0, 2 * side, drain_out, 0)

    def drain_in(t, _):
        hd, lohi = t // 2, lax.rem(t, 2)
        part = pl.ds(pl.multiple_of(lohi * chunk, chunk), chunk)
        landed(dq_hbm.at[part, pl.ds(pl.multiple_of(hd * per_kv, per_kv), per_kv), :], dq_recv.at[hd, lohi])
        landed(dk_in.at[hd, lohi], dk_recv.at[hd, lohi])
        return 0
    lax.fori_loop(0, 4 * side, drain_in, 0)
    def x_wait(d, _):
        x_copy(d).wait_send()
        o = lax.rem(me + d, n_dev)
        landed(xbuf.at[o], x_recv.at[o])
        return 0
    lax.fori_loop(1, n_dev, x_wait, 0)
    dwq_ref[...] = jnp.sum(xbuf[:, 0, :, :], axis=0)
    dwk_ref[...] = jnp.sum(xbuf[:, 1, :, :], axis=0)
    for n, ref in enumerate((dk_ref, dv_ref)):
        for lohi in range(2):
            for h in range(n_groups):
                kst[n, pl.ds(h, chunk, stride=n_groups), :] = dk_in[h, lohi, n].astype(F32)
            ref[lohi * chunk:(lohi + 1) * chunk] = kst[n].reshape(chunk, n_groups, HEAD_DIM).astype(BF16)


def solution(mesh):
    cp_size = mesh.shape['cp']
    side = math.isqrt(cp_size // 2)

    def local_grads(q_raw, k_raw, v_proj, out_fwd, lse_fwd, d_out, q_norm, k_norm):
        local_rows, num_heads = q_raw.shape[0], q_raw.shape[1]
        chunk = local_rows // 2
        kv_heads = k_raw.shape[1]
        per_kv = num_heads // kv_heads
        off_cos, off_sin = rope_tables(np.arange(chunk))
        beg_cos, beg_sin = rope_tables(np.arange(2 * cp_size) * chunk)

        rows = local_rows * per_kv
        dma = pltpu.SemaphoreType.DMA
        any_spec, vmem_spec = pl.BlockSpec(memory_space=pl.ANY), pl.BlockSpec(memory_space=pltpu.VMEM)
        return pl.pallas_call(
            functools.partial(kernel, side, chunk, per_kv),
            out_shape=(jax.ShapeDtypeStruct(q_raw.shape, BF16),
                       jax.ShapeDtypeStruct(k_raw.shape, BF16),
                       jax.ShapeDtypeStruct(k_raw.shape, BF16),
                       jax.ShapeDtypeStruct((1, HEAD_DIM), F32),
                       jax.ShapeDtypeStruct((1, HEAD_DIM), F32)),
            in_specs=[any_spec] * 3 + [vmem_spec] * 9,
            out_specs=(any_spec, vmem_spec, vmem_spec, vmem_spec, vmem_spec),
            scratch_shapes=[
                pltpu.VMEM((side, 2, 2, chunk, HEAD_DIM), F32),
                pltpu.VMEM((side, 2, 2, chunk, HEAD_DIM), F32),
                pltpu.VMEM(q_raw.shape, BF16),
                pltpu.VMEM(q_raw.shape, BF16),
                pltpu.VMEM((kv_heads, 2, 3, chunk, HEAD_DIM), BF16),
                pltpu.VMEM((kv_heads, 2, per_kv, local_rows), F32),
                pltpu.VMEM((3, chunk * kv_heads, HEAD_DIM), F32),
                pltpu.VMEM((kv_heads, 2, 2, chunk, HEAD_DIM), BF16),
                dma((2,)),
                pltpu.VMEM((side, 2, local_rows, per_kv, HEAD_DIM), BF16),
                pltpu.VMEM((side, 2, local_rows, per_kv, HEAD_DIM), BF16),
                pltpu.VMEM((2 * side, side, 2, 3, chunk, HEAD_DIM), BF16),
                pltpu.VMEM((side, 2, 2, per_kv, local_rows), F32),
                pltpu.VMEM((2 * side, rows, HEAD_DIM), BF16),
                pltpu.VMEM((2 * side, rows, HEAD_DIM), BF16),
                pltpu.VMEM((2 * side, HEAD_DIM, rows), BF16),
                pltpu.VMEM((2 * side, HEAD_DIM, rows), BF16),
                pltpu.VMEM((2 * side, rows, HEAD_DIM), F32),
                pltpu.VMEM((2 * side, rows, HEAD_DIM), F32),
                pltpu.VMEM((2 * side, rows, HEAD_DIM), F32),
                pltpu.VMEM((2 * side, side, 2, HEAD_DIM, 2 * chunk), F32),
                pltpu.VMEM((side, 2, side, 2, HEAD_DIM, 2 * chunk), F32),
                pltpu.VMEM((2 * side, rows, HEAD_DIM), F32),
                pltpu.VMEM((side, 2, local_rows, per_kv, HEAD_DIM), BF16),
                pltpu.VMEM((2, side, 2, 2, chunk, HEAD_DIM), BF16),
                pltpu.VMEM((8, HEAD_DIM), F32),
                pltpu.VMEM((8, HEAD_DIM), F32),
                pltpu.VMEM((cp_size, 2, 1, HEAD_DIM), F32),
                dma((3, 2, side)), dma((2, 2, side)), dma((2, side, 2)), dma((side, 2)), dma((side, 2)), dma((side, 2)),
                dma((side, 2, side)), dma((side, 2, side)), dma((2 * side, side)), dma((side, 2, side)),
                dma((side, 2, 2)), dma((kv_heads, 2)), dma((2, side, 2)), dma((kv_heads, 2)),
                dma((cp_size,)), dma((cp_size,)),
            ],
            compiler_params=pltpu.CompilerParams(collective_id=0, has_side_effects=True, vmem_limit_bytes=63 << 20),
            name='attention_backward',
        )(q_raw, d_out, out_fwd, k_raw, v_proj, lse_fwd.T, off_cos, off_sin, beg_cos, beg_sin, q_norm[None, :], k_norm[None, :])

    def grads(*args):
        dq_raw, dk_raw, dv_proj, dq_norm, dk_norm = local_grads(*args)
        return dq_raw, dk_raw, dv_proj, dq_norm[0], dk_norm[0]

    row_spec = P(('dp', 'cp'))
    in_specs = (row_spec, row_spec, row_spec, row_spec, row_spec, row_spec, P(), P())
    out_specs = (row_spec, row_spec, row_spec, P('dp'), P('dp'))
    return jax.shard_map(grads, mesh=mesh, in_specs=in_specs, out_specs=out_specs, check_vma=False)
```
